256 devices in a mesh: seq: 32 (over z, y), tensor: 8 (over x, core).
Axes of the slice: x: 4, y: 4, z: 8, core: 2. Of those that a mesh axis runs over, the one named last changes fastest.
Arguments:
- layer_input: bfloat16 [8192, 4096], P('seq', 'tensor'), may hold values from -6 to 6
- norm_gain: float32 [4096], replicated, may hold values from 0.1 to 1.9
- in_weights: bfloat16 [2, 4096, 2048], P(None, None, 'tensor'), may hold values from -0.09375 to 0.09375
- conv_weight: float32 [4, 2048], P(None, 'tensor'), may hold values from -4 to 4
- conv_bias: float32 [2048], P('tensor'), may hold values from -3 to 3
- gate_weights: bfloat16 [2, 8, 256, 256], P(None, 'tensor'), may hold values from -0.375 to 0.375
- gate_bias: float32 [2, 2048], P(None, 'tensor'), may hold values from -4 to 4
- decay_rate: float32 [2048], P('tensor'), may hold values from 1e-06 to 0.03, as said below
- out_weight: bfloat16 [2048, 4096], P('tensor'), may hold values from -0.1875 to 0.1875
- mlp_gain: float32 [4096], replicated, may hold values from 0.1 to 1.9
- mlp_in: bfloat16 [2, 4096, 6144], P(None, 'seq', 'tensor'), may hold values from -0.09375 to 0.09375
- mlp_out: bfloat16 [6144, 4096], P('tensor', 'seq'), may hold values from -0.15625 to 0.15625
Outputs:
- block_output: bfloat16 [8192, 4096], P('seq', 'tensor')
The draws below stay inside these ranges and needn't reach their ends.
Inputs may be any that keep to these rules, and one draw needn't show every extreme that they name: `decay_rate`: every rate is positive.
All inputs are finite; a program needn't handle non-finite values.
Results may differ from the reference program's by a relative error of at most 0.015.
Values may be sent and summed in bfloat16 or wider, within the bound.
A program may use at most 128 MiB of HBM per device.

```python
import jax
import jax.numpy as jnp
from jax import lax

D = 4096
BW = 256
BLOCKS = 8
LRU = 2048
FF = 6144
TAPS = 4
TOKENS = 8192
N_TENSOR = 8


def draw_decay_rate(key, part):
    first_key = jax.random.fold_in(jax.random.fold_in(key, 7103), 0)
    broad = jnp.exp(jax.random.uniform(first_key, (LRU,), jnp.float32, jnp.log(1e-05), jnp.log(0.03)))
    return broad.astype(jnp.float32)


def strengthened(drawn, stream_key, source, target, blocks, factor):
    def block_of(dim):
        return (jnp.arange(drawn.shape[dim]) // (drawn.shape[dim] // blocks)).reshape((-1,) + (1,) * (drawn.ndim - 1 - dim))

    first = jax.random.permutation(stream_key, blocks)[block_of(target)]
    other_side = (block_of(target) + blocks // 2) % blocks
    return jnp.where((block_of(source) == first) | (block_of(source) == other_side), factor * drawn, drawn)


def block_scale(stream_key, shape, pieces, smallest, top_value):
    factor_of = 1.0
    for axis_at, parts in pieces:
        heights = jax.random.uniform(jax.random.fold_in(jax.random.fold_in(stream_key, 6), axis_at), (parts,), jnp.float32, smallest / len(pieces), top_value / len(pieces))
        factor_of = factor_of * jnp.repeat(jnp.exp(heights), shape[axis_at] // parts).reshape((-1,) + (1,) * (len(shape) - 1 - axis_at))
    return factor_of


def bell_draw(stream_key, shape, spread, most, shards=(), held_as=jnp.bfloat16):
    drawn = spread * jax.random.normal(stream_key, shape, jnp.float32)
    if shards:
        drawn = drawn * block_scale(stream_key, shape, shards, -0.22, 0.18)
    return jnp.clip(drawn, -most, most).astype(held_as)


def bell_draw_with(key, shape, width, most, cuts, heavy, dtype=jnp.bfloat16):
    result = width * jax.random.normal(key, shape, jnp.float32)
    if cuts:
        result = result * block_scale(key, shape, cuts, -0.22, 0.18)
    return jnp.clip(strengthened(result, jax.random.fold_in(key, 3), *heavy), -most, most).astype(dtype)


def setup_inputs(seed: int = 0) -> dict:
    keys = jax.random.split(jax.random.key(seed), 13)
    layer_input = bell_draw(keys[0], (TOKENS, D), 1.0, 6.0, ((0, 32), (1, 8)))
    norm_gain = jnp.clip(1.0 + 0.18 * jax.random.normal(keys[1], (D,), jnp.float32), 0.1, 1.9)
    in_weights = bell_draw(keys[2], (2, D, LRU), D ** -0.5, 0.09375, ((2, 8),))
    conv_weight = bell_draw(keys[3], (TAPS, LRU), 1.0, 4.0, ((1, 8),), jnp.float32)
    conv_bias = bell_draw(keys[4], (LRU,), 0.5, 3.0, ((0, 8),), jnp.float32)
    gate_weights = bell_draw(keys[5], (2, BLOCKS, BW, BW), BW ** -0.5, 0.375, ((1, 8),))
    gate_bias = bell_draw(keys[6], (2, LRU), 1.0, 4.0, ((1, 8),), jnp.float32)
    decay_rate = draw_decay_rate(jax.random.fold_in(keys[12], 71), 0)
    out_weight = bell_draw_with(keys[8], (LRU, D), LRU ** -0.5, 0.1875, ((0, 8),), (0, 1, 8, 2.0))
    mlp_gain = jnp.clip(1.0 + 0.18 * jax.random.normal(keys[9], (D,), jnp.float32), 0.1, 1.9)
    mlp_in = bell_draw(keys[10], (2, D, FF), D ** -0.5, 0.09375, ((1, 32), (2, 8)))
    mlp_out = bell_draw_with(keys[11], (FF, D), FF ** -0.5, 0.15625, ((0, 8), (1, 32)), (0, 1, 32, 2.75))
    return dict(layer_input=layer_input, norm_gain=norm_gain, in_weights=in_weights, conv_weight=conv_weight, conv_bias=conv_bias, gate_weights=gate_weights, gate_bias=gate_bias, decay_rate=decay_rate, out_weight=out_weight, mlp_gain=mlp_gain, mlp_in=mlp_in, mlp_out=mlp_out)


def rms_scale(rows, gain):
    values = rows.astype(jnp.float32)
    mean_square = lax.optimization_barrier(jnp.mean(values * values, axis=-1, keepdims=True))
    return (values * lax.rsqrt(mean_square + 1e-06) * gain).astype(jnp.bfloat16)

def advance(state, inputs):
    decay, driven = inputs
    state = decay * state + driven
    return (state, state)

def reference(layer_input, norm_gain, in_weights, conv_weight, conv_bias, gate_weights, gate_bias, decay_rate, out_weight, mlp_gain, mlp_in, mlp_out):
    normed = rms_scale(layer_input, norm_gain)
    branch_x = jnp.dot(normed, in_weights[0], preferred_element_type=jnp.float32).astype(jnp.bfloat16)
    branch_y = jax.nn.gelu(jnp.dot(normed, in_weights[1], preferred_element_type=jnp.float32), approximate=True)
    padded = jnp.concatenate([jnp.zeros((TAPS - 1, LRU), jnp.bfloat16), branch_x], axis=0).astype(jnp.float32)
    convolved = jnp.zeros((TOKENS, LRU), jnp.float32) + conv_bias
    for tap_index in range(TAPS):
        start_row = TAPS - 1 - tap_index
        convolved = convolved + conv_weight[tap_index] * padded[start_row:start_row + TOKENS]
    conv_out = convolved.astype(jnp.bfloat16)
    blocks_in = conv_out.astype(jnp.float32).reshape(TOKENS, BLOCKS, BW)
    gate_pre = jnp.einsum('tnc,knce->ktne', blocks_in, gate_weights.astype(jnp.float32)).reshape(2, TOKENS, LRU) + gate_bias[:, None, :]
    log_decay = -8.0 * jax.nn.sigmoid(gate_pre[0]) * decay_rate
    decay = jnp.exp(log_decay)
    driven = conv_out.astype(jnp.float32) * jax.nn.sigmoid(gate_pre[1]) * jnp.sqrt(-jnp.expm1(2.0 * log_decay))
    _, states = lax.scan(advance, jnp.zeros((LRU,), jnp.float32), (decay, driven))
    mixed = (states * branch_y).astype(jnp.bfloat16)
    group = LRU // N_TENSOR
    rec_sum = jnp.zeros((TOKENS, D), jnp.float32)
    for group_index in range(N_TENSOR):
        term = jnp.dot(mixed[:, group_index * group:(group_index + 1) * group], out_weight[group_index * group:(group_index + 1) * group], preferred_element_type=jnp.float32).astype(jnp.bfloat16)
        term = lax.optimization_barrier(term)
        rec_sum = rec_sum + term.astype(jnp.float32)
    residual = (layer_input.astype(jnp.float32) + rec_sum).astype(jnp.bfloat16)
    mlp_normed = rms_scale(residual, mlp_gain)
    gate = jnp.dot(mlp_normed, mlp_in[0], preferred_element_type=jnp.float32)
    upward = jnp.dot(mlp_normed, mlp_in[1], preferred_element_type=jnp.float32)
    hidden = (jax.nn.gelu(gate, approximate=True) * upward).astype(jnp.bfloat16)
    down = jnp.dot(hidden, mlp_out, preferred_element_type=jnp.float32)
    return (residual.astype(jnp.float32) + down).astype(jnp.bfloat16)
```

```python
import functools

import jax
import jax.numpy as jnp
from jax import lax
from jax.experimental import pallas as pl
from jax.experimental.pallas import tpu as pltpu
from jax.sharding import PartitionSpec as P

NY = 4
NX = 4
EPS = 1e-06
F32 = jnp.float32
BF16 = jnp.bfloat16
MESSAGES = 200


def mod(value, size):
    return lax.rem(value + size, size)


def expm1_negated(v):
    series = 1.0 + v * (1.0 / 9.0)
    for n in range(8, 1, -1):
        series = 1.0 + v * (1.0 / n) * series
    return jnp.where(v > -0.5, -v * series, 1.0 - jnp.exp(v))


class Wire:
    def __init__(self, send, recv):
        self.send, self.recv, self.used, self.open = send, recv, 0, []

    def message(self, src, dst, landing, device):
        self.used += 1
        return Message(self, self.used - 1, src, dst, landing, device)

    def drain(self):
        for message in self.open:
            message.copy(message.dst).wait_send()


class Message:
    def __init__(self, wire, number, src, dst, landing, device):
        self.wire, self.number, self.src, self.dst, self.landing, self.device = (
            wire, number, src, dst, landing, device,
        )

    def copy(self, dst):
        return pltpu.make_async_remote_copy(
            src_ref=self.src,
            dst_ref=dst,
            send_sem=self.wire.send.at[self.number],
            recv_sem=self.wire.recv.at[self.number],
            device_id=self.device,
            device_id_type=pl.DeviceIdType.MESH,
        )

    def start(self):
        self.copy(self.dst).start()
        self.wire.open.append(self)

    def arrived(self):
        self.copy(self.landing).wait_recv()


class Spread:
    def __init__(self, wire, piece, me, device_of, own=None):
        nxt, prv, opp = mod(me + 1, 4), mod(me + 3, 4), mod(me + 2, 4)
        own = own or (lambda h: piece(me, h))
        self.na = wire.message(own(0), piece(me, 0), piece(prv, 0), device_of(nxt))
        self.nb = wire.message(own(1), piece(me, 1), piece(prv, 1), device_of(nxt))
        self.pb = wire.message(own(1), piece(me, 1), piece(nxt, 1), device_of(prv))
        self.pa = wire.message(own(0), piece(me, 0), piece(nxt, 0), device_of(prv))
        self.fn = wire.message(piece(prv, 0), piece(prv, 0), piece(opp, 0), device_of(nxt))
        self.fp = wire.message(piece(nxt, 1), piece(nxt, 1), piece(opp, 1), device_of(prv))

    def start(self):
        self.na.start()
        self.pb.start()
        self.nb.start()
        self.pa.start()

    def forward(self):
        self.na.arrived()
        self.fn.start()
        self.pb.arrived()
        self.fp.start()

    def prv_done(self):
        self.nb.arrived()

    def nxt_done(self):
        self.pa.arrived()

    def opp_done(self):
        self.fn.arrived()
        self.fp.arrived()


class Gathered:
    def __init__(self, wire, part, me, device_of, box):
        nxt, prv, opp = mod(me + 1, 4), mod(me + 3, 4), mod(me + 2, 4)
        self.part, self.me, self.nxt, self.prv, self.box = part, me, nxt, prv, box
        def send(src, slot, device):
            return wire.message(src, box.at[slot], box.at[slot], device)
        self.oa = send(part(opp, 0), 0, device_of(nxt))
        self.ob = send(part(opp, 1), 1, device_of(prv))
        self.db = send(part(nxt, 1), 2, device_of(nxt))
        self.da = send(part(prv, 0), 3, device_of(prv))
        self.ca = send(part(nxt, 0), 4, device_of(nxt))
        self.cb = send(part(prv, 1), 5, device_of(prv))

    def start_far(self):
        self.oa.start()
        self.ob.start()

    def start_next(self):
        self.db.start()

    def start_prev(self):
        self.da.start()

    def relay(self):
        for arriving, leaving, member, half, slot in (
            (self.oa, self.ca, self.nxt, 0, 0),
            (self.ob, self.cb, self.prv, 1, 1),
        ):
            arriving.arrived()
            ref = self.part(member, half)
            ref[...] = (ref[...].astype(F32) + self.box[slot].astype(F32)).astype(BF16)
            leaving.start()

    def result(self):
        self.da.arrived()
        self.ca.arrived()
        self.db.arrived()
        self.cb.arrived()
        halves = []
        for half, slots in ((0, (4, 3)), (1, (2, 5))):
            value = self.part(self.me, half)[...].astype(F32)
            for slot in slots:
                value = value + self.box[slot].astype(F32)
            halves.append(value)
        return halves


def picked(k, values):
    result = values[0]
    for n in range(1, len(values)):
        result = jnp.where(k == n, values[n], result)
    return result


def kernel(
    nz, x_ref, ng_ref, cw_ref, cb_ref, gw_ref, gb_ref, dr_ref, mg_ref, inw_hbm, outw_hbm, mi_hbm, mo_hbm, o_ref,
    xg, inw, outw, mi, wsrc, wt, acc, ss, bxs, tail, ytab, ztab, mixed, op, oi, obox, res,
    xt, acc2, ss2, hid, po, abox, bbox, abox2, bbox2, give, got, send_sem, recv_sem, local_sem,
):
    tm, cw = x_ref.shape
    hm = tm // 2
    ch = bxs.shape[1]
    d = ng_ref.shape[1]
    rm = tm // 2
    ff = wsrc.shape[1] // NY
    lanes = d // (nz * NY)
    zl = NY * lanes
    nseq = nz * NY

    s = lax.axis_index("seq")
    t = lax.axis_index("tensor")
    z, y = lax.div(s, NY), lax.rem(s, NY)
    x, c = lax.div(t, 2), lax.rem(t, 2)

    def dev(z_=None, y_=None, x_=None, c_=None):
        z_, y_ = (z if z_ is None else z_), (y if y_ is None else y_)
        x_, c_ = (x if x_ is None else x_), (c if c_ is None else c_)
        return (z_ * NY + y_, x_ * 2 + c_)

    along_x = lambda i: dev(x_=i)
    along_y = lambda j: dev(y_=j)
    sibling = dev(c_=1 - c)
    xn, xp, xo = mod(x + 1, NX), mod(x + 3, NX), mod(x + 2, NX)
    yn, yp, yo = mod(y + 1, NY), mod(y + 3, NY), mod(y + 2, NY)
    after, before = (mod(s + 1, nseq), t), (mod(s + nseq - 1, nseq), t)

    loads = {}
    for number, (name, src, dst) in enumerate(
        (("inw", inw_hbm, inw), ("outw", outw_hbm, outw), ("mi", mi_hbm, mi), ("mo", mo_hbm, wsrc.at[2]))
    ):
        loads[name] = pltpu.make_async_copy(src, dst, local_sem.at[number])
    for name in ("mi", "mo", "inw", "outw"):
        loads[name].start()

    barrier = pltpu.get_barrier_semaphore()
    partners = [dev(x_=xn), dev(x_=xp), sibling, after, before]
    partners += [dev(y_=mod(y + k, NY)) for k in range(1, NY)]
    partners += [dev(z_=mod(z + k, nz)) for k in range(1, nz)]
    for partner in partners:
        pl.semaphore_signal(barrier, inc=1, device_id=partner, device_id_type=pl.DeviceIdType.MESH)
    pl.semaphore_wait(barrier, len(partners))

    wire = Wire(send_sem, recv_sem)

    def x_piece(i, h):
        return xg.at[i * 2 + c, pl.ds(h * hm, hm)]

    xring = Spread(wire, x_piece, x, along_x, own=lambda h: x_ref.at[pl.ds(h * hm, hm)])
    xring.start()
    to_sib = {}
    for name, i in (("own", x), ("prv", xp), ("nxt", xn), ("opp", xo)):
        src = x_ref if name == "own" else xg.at[i * 2 + c]
        to_sib[name] = wire.message(src, xg.at[i * 2 + c], xg.at[i * 2 + 1 - c], sibling)
    to_sib["own"].start()
    xg[t] = x_ref[...]

    loads["mi"].wait()
    for g in range(2):
        wsrc[g] = mi[g].astype(F32).T.astype(BF16)
    loads["mo"].wait()

    def w_rows(j):
        return wsrc.at[:, pl.ds(pl.multiple_of(j * ff, 16), ff)]

    def w_lanes(slot, start, size):
        return wt.at[:, pl.ds(slot * ff, ff), pl.ds(pl.multiple_of(start, 128), size)]

    w_over_y = []
    for k in range(1, NY):
        j, src_y = mod(y + k, NY), mod(y + NY - k, NY)
        message = wire.message(
            w_rows(j), w_lanes(0, s * lanes, lanes), w_lanes(0, (z * NY + src_y) * lanes, lanes), along_y(j)
        )
        message.start()
        w_over_y.append(message)
    wt[:, pl.ds(0, ff), pl.ds(pl.multiple_of(s * lanes, 128), lanes)] = wsrc[:, pl.ds(pl.multiple_of(y * ff, 16), ff)]

    zn, zp = mod(z + 1, nz), mod(z + nz - 1, nz)
    steps = nz // 2
    z_up, z_down, w_sib = [], [], []
    for k in range(1, steps + 1):
        half = zl // 2 if k == steps else zl
        up, up_in = mod(z + nz - (k - 1), nz) * zl, mod(z + nz - k, nz) * zl
        down, down_in = mod(z + k - 1, nz) * zl, mod(z + k, nz) * zl
        shift = zl - half
        z_up.append(wire.message(w_lanes(0, up, half), w_lanes(0, up, half), w_lanes(0, up_in, half), dev(z_=zn)))
        z_down.append(
            wire.message(
                w_lanes(0, down + shift, half), w_lanes(0, down + shift, half), w_lanes(0, down_in + shift, half),
                dev(z_=zp),
            )
        )

    def w_to_sib(start, size):
        w_sib.append(wire.message(w_lanes(0, start, size), w_lanes(1, start, size), w_lanes(1, start, size), sibling))

    w_to_sib(z * zl, zl)
    for k in range(1, steps + 1):
        half = zl // 2 if k == steps else zl
        w_to_sib(mod(z + nz - k, nz) * zl, half)
        w_to_sib(mod(z + k, nz) * zl + zl - half, half)

    def weights_begin():
        for message in w_over_y:
            message.arrived()
        z_up[0].start()
        z_down[0].start()
        w_sib[0].start()

    def weights_step(k):
        z_up[k - 1].arrived()
        if k < steps:
            z_up[k].start()
        z_down[k - 1].arrived()
        if k < steps:
            z_down[k].start()
        w_sib[2 * k - 1].start()
        w_sib[2 * k].start()

    acc[...] = jnp.zeros_like(acc)
    ss[...] = jnp.zeros_like(ss)
    loads["inw"].wait()
    order = [t, x * 2 + 1 - c, xp * 2 + c, xn * 2 + c, xp * 2 + 1 - c, xn * 2 + 1 - c, xo * 2 + c, xo * 2 + 1 - c]

    def step_2():
        xring.forward()
        xring.prv_done()
        to_sib["prv"].start()

    def step_3():
        xring.nxt_done()
        to_sib["nxt"].start()

    def step_6():
        xring.opp_done()
        to_sib["opp"].start()

    arrivals = {
        1: to_sib["own"].arrived,
        2: step_2,
        3: step_3,
        4: to_sib["prv"].arrived,
        5: to_sib["nxt"].arrived,
        6: step_6,
        7: to_sib["opp"].arrived,
    }

    def take(k, _):
        for at, step in arrivals.items():
            pl.when(k == at)(step)
        b = picked(k, order)
        at = pl.multiple_of(b * cw, 128)
        block = xg[b].astype(F32)
        ss[...] += jnp.sum(block * block, axis=1, keepdims=True)
        scaled = (block * ng_ref[:, pl.ds(at, cw)]).astype(BF16)
        for g in range(2):
            acc[g] += jnp.dot(scaled, inw[g, pl.ds(at, cw)], preferred_element_type=F32)
        return 0

    lax.fori_loop(0, 8, take, 0)
    scale = lax.rsqrt(ss[...] * (1.0 / d) + EPS)
    bxs[...] = (acc[0] * scale).astype(BF16)
    tails = wire.message(bxs.at[pl.ds(tm - 16, 16)], tail, tail, after)
    tails.start()
    weights_begin()
    branch_y = jax.nn.gelu(acc[1] * scale, approximate=True)
    acc[1] = branch_y

    tails.arrived()
    earlier = jnp.where(s > 0, tail[...].astype(F32), 0.0)
    padded = jnp.concatenate([earlier, bxs[...].astype(F32)], axis=0)
    convolved = jnp.zeros((tm, ch), F32) + cb_ref[...]
    for k in range(cw_ref.shape[0]):
        convolved = convolved + cw_ref[k : k + 1] * pltpu.roll(padded, k, 0)[16:]
    conv_out = convolved.astype(BF16)
    gates = [
        jnp.dot(conv_out, gw_ref[g, 0], preferred_element_type=F32) + gb_ref[g : g + 1] for g in range(2)
    ]
    log_decay = -8.0 * jax.nn.sigmoid(gates[0]) * dr_ref[...]
    decay = jnp.exp(log_decay)
    driven = conv_out.astype(F32) * jax.nn.sigmoid(gates[1]) * jnp.sqrt(expm1_negated(2.0 * log_decay))
    row = lax.broadcasted_iota(jnp.int32, (tm, ch), 0)
    step = 1
    while step < tm:
        inside = row >= step
        driven = driven + decay * jnp.where(inside, pltpu.roll(driven, step, 0), 0.0)
        decay = decay * jnp.where(inside, pltpu.roll(decay, step, 0), 1.0)
        step *= 2
    ytab[y, 0:1] = decay[tm - 1 :]
    ytab[y, 1:2] = driven[tm - 1 :]
    over_y = []
    for k in range(1, NY):
        over_y.append(
            wire.message(ytab.at[y], ytab.at[y], ytab.at[mod(y + NY - k, NY)], along_y(mod(y + k, NY)))
        )
        over_y[-1].start()
    for message in over_y:
        message.arrived()
    total_a, total_b = jnp.ones((1, ch), F32), jnp.zeros((1, ch), F32)
    before_a, before_b = total_a, total_b
    for j in range(NY):
        a, b = ytab[j, 0:1], ytab[j, 1:2]
        before_b = jnp.where(j < y, a * before_b + b, before_b)
        before_a = jnp.where(j < y, a * before_a, before_a)
        total_b = a * total_b + b
        total_a = a * total_a
    ztab[z, 0:1] = total_a
    ztab[z, 1:2] = total_b
    over_z = []
    for k in range(1, nz):
        over_z.append(
            wire.message(ztab.at[z], ztab.at[z], ztab.at[mod(z + nz - k, nz)], dev(z_=mod(z + k, nz)))
        )
        over_z[-1].start()
    for message in over_z:
        message.arrived()
    carry = jnp.zeros((1, ch), F32)
    for j in range(nz):
        carry = jnp.where(j < z, ztab[j, 0:1] * carry + ztab[j, 1:2], carry)
    carry = before_a * carry + before_b
    mixed[...] = ((decay * carry + driven) * acc[1]).astype(BF16)
    if steps > 1:
        weights_step(1)

    loads["outw"].wait()
    columns = (xo, xn, xp, x)

    def block(i):
        return pl.ds(pl.multiple_of(i * cw, 128), cw)

    over_d2d = []
    for n, i in enumerate(columns):
        for core in (1 - c, c):
            at = pl.multiple_of((i * 2 + core) * cw, 128)
            part = jnp.dot(mixed[...], outw[:, pl.ds(at, cw)], preferred_element_type=F32)
            op[core, :, block(i)] = part.astype(BF16)
            if core is not c:
                over_d2d.append(wire.message(op.at[1 - c, :, block(i)], oi.at[n], oi.at[n], sibling))
                over_d2d[-1].start()

    out_ring = Gathered(wire, lambda i, h: op.at[c, pl.ds(h * hm, hm), block(i)], x, along_x, obox)
    starts = (out_ring.start_far, out_ring.start_next, out_ring.start_prev, lambda: None)
    for n, i in enumerate(columns):
        over_d2d[n].arrived()
        op[c, :, block(i)] = (op[c, :, block(i)].astype(F32) + oi[n].astype(F32)).astype(BF16)
        starts[n]()
    out_ring.relay()
    for h, value in enumerate(out_ring.result()):
        rows = pl.ds(h * hm, hm)
        res[rows] = (x_ref[rows].astype(F32) + value).astype(BF16)

    def token(j, h=None):
        if h is None:
            return pl.ds(pl.multiple_of(j * rm, 16), rm)
        return pl.ds(pl.multiple_of(j * rm + h * (rm // 2), 16), rm // 2)

    mine, theirs = pl.ds(pl.multiple_of(c * rm, 16), rm), pl.ds(pl.multiple_of((1 - c) * rm, 16), rm)
    swap = wire.message(
        res.at[theirs], xt.at[c, token(y), block(x)], xt.at[1 - c, token(y), block(x)], sibling,
    )
    swap.start()
    xt[c, token(y), block(x)] = res[mine]
    other = 1 - c
    a_x = Spread(wire, lambda i, h: xt.at[c, token(y, h), block(i)], x, along_x)
    a_y = [
        Spread(wire, lambda j, h, i=i: xt.at[c, token(j, h), block(i)], y, along_y) for i in (x, xp, xn, xo)
    ]
    b_y = Spread(wire, lambda j, h: xt.at[other, token(j, h), block(x)], y, along_y)
    b_x = [
        Spread(wire, lambda i, h, j=j: xt.at[other, token(j, h), block(i)], x, along_x) for j in (y, yp, yn, yo)
    ]
    a_x.start()
    a_y[0].start()
    if steps > 2:
        weights_step(2)
    swap.arrived()
    b_y.start()
    b_x[0].start()
    a_x.forward()
    b_y.forward()
    a_x.prv_done()
    a_y[1].start()
    b_y.prv_done()
    b_x[1].start()
    a_x.nxt_done()
    a_y[2].start()
    b_y.nxt_done()
    b_x[2].start()
    a_y[0].forward()
    b_x[0].forward()
    a_x.opp_done()
    a_y[3].start()
    b_y.opp_done()
    b_x[3].start()
    for k in range(3, steps):
        weights_step(k)
    acc2[...] = jnp.zeros_like(acc2)
    ss2[...] = jnp.zeros_like(ss2)

    def ring_done(ring):
        ring.prv_done()
        ring.nxt_done()
        ring.opp_done()

    def rows_0():
        a_y[1].forward()
        b_x[1].forward()
        ring_done(a_y[0])
        weights_step(steps)
        for message in w_sib:
            message.arrived()

    def rows_1():
        a_y[2].forward()
        b_x[2].forward()

    def rows_2():
        a_y[3].forward()
        b_x[3].forward()
        ring_done(a_y[1])

    def rows_3():
        ring_done(a_y[2])

    def rows_4():
        for ring in b_x:
            ring.prv_done()

    def rows_5():
        for ring in b_x:
            ring.nxt_done()

    def rows_6():
        ring_done(a_y[3])

    def rows_7():
        for ring in b_x:
            ring.opp_done()

    row_steps = (rows_0, rows_1, rows_2, rows_3, rows_4, rows_5, rows_6, rows_7)
    which = ((c, x), (other, x), (c, xp), (c, xn), (other, xp), (other, xn), (c, xo), (other, xo))

    def multiply(k, _):
        for at, step in enumerate(row_steps):
            pl.when(k == at)(step)
        core, i = picked(k, [w[0] for w in which]), picked(k, [w[1] for w in which])
        at = pl.multiple_of((i * 2 + core) * cw, 128)
        rows = xt[core, :, block(i)].astype(F32)
        ss2[...] += jnp.sum(rows * rows, axis=1, keepdims=True)
        scaled = (rows * mg_ref[:, pl.ds(at, cw)]).astype(BF16)
        for g in range(2):
            acc2[g] += lax.dot_general(
                scaled, wt[g, :, pl.ds(at, cw)], (((1,), (1,)), ((), ())), preferred_element_type=F32
            )
        return 0

    lax.fori_loop(0, 8, multiply, 0)
    scale2 = lax.rsqrt(ss2[...] * (1.0 / d) + EPS)
    hid[...] = (jax.nn.gelu(acc2[0] * scale2, approximate=True) * (acc2[1] * scale2)).astype(BF16)

    a_back = [
        Gathered(wire, lambda j, h, i=i: po.at[c, token(j, h), block(i)], y, along_y, abox.at[n])
        for n, i in enumerate(columns)
    ]
    b_rows = (yo, yn, yp, y)
    b_back = [
        Gathered(wire, lambda i, h, j=j: po.at[other, token(j, h), block(i)], x, along_x, bbox.at[n])
        for n, j in enumerate(b_rows)
    ]
    a_last = Gathered(wire, lambda i, h: po.at[c, token(y, h), block(i)], x, along_x, abox2)
    b_last = Gathered(wire, lambda j, h: po.at[other, token(j, h), block(x)], y, along_y, bbox2)

    def down_block(core, i):
        at = pl.multiple_of((i * 2 + core) * cw, 128)
        part = jnp.dot(hid[...], wt[2, :, pl.ds(at, cw)], preferred_element_type=F32)
        po[core, :, block(i)] = part.astype(BF16)

    def a_all(n):
        a_back[n].start_far()
        a_back[n].start_next()
        a_back[n].start_prev()

    def b_all(method):
        for ring in b_back:
            getattr(ring, method)()

    down_steps = {
        0: lambda: a_all(0),
        1: lambda: b_all("start_far"),
        2: lambda: a_all(1),
        3: lambda: b_all("start_next"),
        4: lambda: a_all(2),
        5: lambda: b_all("start_prev"),
        6: lambda: a_all(3),
    }

    def down(k, _):
        down_block(picked(lax.rem(k, 2), [c, other]), picked(lax.div(k, 2), list(columns)))
        for at, step in down_steps.items():
            pl.when(k == at)(step)
        return 0

    lax.fori_loop(0, 8, down, 0)

    a_starts = (a_last.start_far, a_last.start_next, a_last.start_prev, lambda: None)
    b_starts = (b_last.start_far, b_last.start_next, b_last.start_prev, lambda: None)
    for n in range(4):
        a_back[n].relay()
        b_back[n].relay()
    for n in range(4):
        for ring, start, core, rows_at, i in (
            (a_back[n], a_starts[n], c, y, columns[n]),
            (b_back[n], b_starts[n], other, b_rows[n], x),
        ):
            for h, value in enumerate(ring.result()):
                po[core, token(rows_at, h), block(i)] = value.astype(BF16)
            start()
    b_last.relay()
    a_last.relay()
    for h, value in enumerate(b_last.result()):
        give[pl.ds(h * (rm // 2), rm // 2)] = value.astype(BF16)
    back = wire.message(give, got, got, sibling)
    back.start()
    for h, value in enumerate(a_last.result()):
        rows = pl.ds(pl.multiple_of(c * rm + h * (rm // 2), 16), rm // 2)
        o_ref[rows] = (res[rows].astype(F32) + value).astype(BF16)
    back.arrived()
    o_ref[theirs] = (res[theirs].astype(F32) + got[...].astype(F32)).astype(BF16)
    wire.drain()


def shards(
    nz, layer_input, norm_gain, in_weights, conv_weight, conv_bias, gate_weights, gate_bias, decay_rate, out_weight,
    mlp_gain, mlp_in, mlp_out,
):
    tm, cw = layer_input.shape
    d, ch = in_weights.shape[1:]
    units = mlp_out.shape[0]
    ff = units // NY
    rm = tm // 2
    vmem = pl.BlockSpec(memory_space=pltpu.VMEM)
    hbm = pl.BlockSpec(memory_space=pl.ANY)
    scratch = [
        ((8, tm, cw), BF16),
        ((2, d, ch), BF16),
        ((ch, d), BF16),
        (mlp_in.shape, BF16),
        ((3, units, mlp_in.shape[1]), BF16),
        ((3, 2 * ff, d), BF16),
        ((2, tm, ch), F32),
        ((tm, 1), F32),
        ((tm, ch), BF16),
        ((16, ch), BF16),
        ((NY, 2, ch), F32),
        ((nz, 2, ch), F32),
        ((tm, ch), BF16),
        ((2, tm, NX * cw), BF16),
        ((4, tm, cw), BF16),
        ((6, tm // 2, cw), BF16),
        ((tm, cw), BF16),
        ((2, NY * rm, NX * cw), BF16),
        ((2, NY * rm, 2 * ff), F32),
        ((NY * rm, 1), F32),
        ((NY * rm, 2 * ff), BF16),
        ((2, NY * rm, NX * cw), BF16),
        ((4, 6, rm // 2, cw), BF16),
        ((4, 6, rm // 2, cw), BF16),
        ((6, rm // 2, cw), BF16),
        ((6, rm // 2, cw), BF16),
        ((rm, cw), BF16),
        ((rm, cw), BF16),
    ]
    call = pl.pallas_call(
        functools.partial(kernel, nz),
        out_shape=jax.ShapeDtypeStruct((tm, cw), BF16),
        in_specs=[vmem] * 8 + [hbm] * 4,
        out_specs=vmem,
        scratch_shapes=[pltpu.VMEM(shape, dtype) for shape, dtype in scratch]
        + [
            pltpu.SemaphoreType.DMA((MESSAGES,)),
            pltpu.SemaphoreType.DMA((MESSAGES,)),
            pltpu.SemaphoreType.DMA((4,)),
        ],
        compiler_params=pltpu.CompilerParams(
            collective_id=0, has_side_effects=True, vmem_limit_bytes=56 * 1024 * 1024
        ),
    )
    return call(
        layer_input, norm_gain[None], conv_weight, conv_bias[None], gate_weights, gate_bias, decay_rate[None],
        mlp_gain[None], in_weights, out_weight, mlp_in, mlp_out,
    )


def solution(mesh):
    return jax.shard_map(
        functools.partial(shards, mesh.shape["seq"] // NY),
        mesh=mesh,
        in_specs=(
            P("seq", "tensor"),
            P(),
            P(None, None, "tensor"),
            P(None, "tensor"),
            P("tensor"),
            P(None, "tensor", None, None),
            P(None, "tensor"),
            P("tensor"),
            P("tensor", None),
            P(),
            P(None, "seq", "tensor"),
            P("tensor", "seq"),
        ),
        out_specs=P("seq", "tensor"),
        check_vma=False,
    )
```

```python
import functools

import jax
import jax.numpy as jnp
from jax import lax
from jax.experimental import pallas as pl
from jax.experimental.pallas import tpu as pltpu
from jax.sharding import PartitionSpec as P

NY = 4
NX = 4
EPS = 1e-06
F32 = jnp.float32
BF16 = jnp.bfloat16
MESSAGES = 224
RIM = 8


def mod(value, size):
    return lax.rem(value + size, size)


def expm1_negated(v):
    series = 1.0 + v * (1.0 / 9.0)
    for n in range(8, 1, -1):
        series = 1.0 + v * (1.0 / n) * series
    return jnp.where(v > -0.5, -v * series, 1.0 - jnp.exp(v))


class Wire:
    def __init__(self, send, recv):
        self.send, self.recv, self.used, self.open = send, recv, 0, []

    def message(self, src, dst, landing, device):
        self.used += 1
        return Message(self, self.used - 1, src, dst, landing, device)

    def drain(self):
        for message in self.open:
            message.copy(message.dst).wait_send()


class Message:
    def __init__(self, wire, number, src, dst, landing, device):
        self.wire, self.number, self.src, self.dst, self.landing, self.device = (
            wire, number, src, dst, landing, device,
        )

    def copy(self, dst):
        return pltpu.make_async_remote_copy(
            src_ref=self.src,
            dst_ref=dst,
            send_sem=self.wire.send.at[self.number],
            recv_sem=self.wire.recv.at[self.number],
            device_id=self.device,
            device_id_type=pl.DeviceIdType.MESH,
        )

    def start(self):
        self.copy(self.dst).start()
        self.wire.open.append(self)

    def arrived(self):
        self.copy(self.landing).wait_recv()


class Spread:
    def __init__(self, wire, piece, me, device_of, own=None):
        nxt, prv, opp = mod(me + 1, 4), mod(me + 3, 4), mod(me + 2, 4)
        own = own or (lambda h: piece(me, h))
        self.na = wire.message(own(0), piece(me, 0), piece(prv, 0), device_of(nxt))
        self.nb = wire.message(own(1), piece(me, 1), piece(prv, 1), device_of(nxt))
        self.pb = wire.message(own(1), piece(me, 1), piece(nxt, 1), device_of(prv))
        self.pa = wire.message(own(0), piece(me, 0), piece(nxt, 0), device_of(prv))
        self.fn = wire.message(piece(prv, 0), piece(prv, 0), piece(opp, 0), device_of(nxt))
        self.fp = wire.message(piece(nxt, 1), piece(nxt, 1), piece(opp, 1), device_of(prv))

    def start(self):
        self.na.start()
        self.pb.start()
        self.nb.start()
        self.pa.start()

    def forward(self):
        self.na.arrived()
        self.fn.start()
        self.pb.arrived()
        self.fp.start()

    def prv_done(self):
        self.nb.arrived()

    def nxt_done(self):
        self.pa.arrived()

    def opp_done(self):
        self.fn.arrived()
        self.fp.arrived()


class Gathered:
    def __init__(self, wire, part, me, device_of, box):
        nxt, prv, opp = mod(me + 1, 4), mod(me + 3, 4), mod(me + 2, 4)
        self.part, self.me, self.nxt, self.prv, self.box = part, me, nxt, prv, box
        def send(src, slot, device):
            return wire.message(src, box.at[slot], box.at[slot], device)
        self.oa = send(part(opp, 0), 0, device_of(nxt))
        self.ob = send(part(opp, 1), 1, device_of(prv))
        self.db = send(part(nxt, 1), 2, device_of(nxt))
        self.da = send(part(prv, 0), 3, device_of(prv))
        self.ca = send(part(nxt, 0), 4, device_of(nxt))
        self.cb = send(part(prv, 1), 5, device_of(prv))

    def start_far(self):
        self.oa.start()
        self.ob.start()

    def start_next(self):
        self.db.start()

    def start_prev(self):
        self.da.start()

    def relay(self):
        for arriving, leaving, member, half, slot in (
            (self.oa, self.ca, self.nxt, 0, 0),
            (self.ob, self.cb, self.prv, 1, 1),
        ):
            arriving.arrived()
            ref = self.part(member, half)
            ref[...] = (ref[...].astype(F32) + self.box[slot].astype(F32)).astype(BF16)
            leaving.start()

    def result(self):
        self.da.arrived()
        self.ca.arrived()
        self.db.arrived()
        self.cb.arrived()
        halves = []
        for half, slots in ((0, (4, 3)), (1, (2, 5))):
            value = self.part(self.me, half)[...].astype(F32)
            for slot in slots:
                value = value + self.box[slot].astype(F32)
            halves.append(value)
        return halves


def lane_sums(value):
    return sum(value[:, at : at + 128] for at in range(128, value.shape[1], 128)) + value[:, :128]


def picked(k, values):
    result = values[0]
    for n in range(1, len(values)):
        result = jnp.where(k == n, values[n], result)
    return result


def kernel(
    nz, x_ref, ng_ref, cw_ref, cb_ref, gw_ref, gb_ref, dr_ref, mg_ref, inw_hbm, outw_hbm, mi_hbm, mo_hbm, o_ref,
    xg, inw, outw, mi, wsrc, wt, acc, ss, ytab, ztab, mixed, op, oi, obox, res,
    xt, acc2, ss2, hid, po, abox, bbox, abox2, bbox2, give, got, send_sem, recv_sem, local_sem,
):
    tm, cw = x_ref.shape
    hm = tm // 2
    ch = gw_ref.shape[2]
    d = ng_ref.shape[1]
    rm = tm // 2
    ff = wsrc.shape[1] // NY
    lanes = d // (nz * NY)
    zl = NY * lanes
    nseq = nz * NY
    main = pl.ds(RIM, tm)

    s = lax.axis_index("seq")
    t = lax.axis_index("tensor")
    z, y = lax.div(s, NY), lax.rem(s, NY)
    x, c = lax.div(t, 2), lax.rem(t, 2)

    def dev(z_=None, y_=None, x_=None, c_=None):
        z_, y_ = (z if z_ is None else z_), (y if y_ is None else y_)
        x_, c_ = (x if x_ is None else x_), (c if c_ is None else c_)
        return (z_ * NY + y_, x_ * 2 + c_)

    along_x = lambda i: dev(x_=i)
    along_y = lambda j: dev(y_=j)
    sibling = dev(c_=1 - c)
    xn, xp, xo = mod(x + 1, NX), mod(x + 3, NX), mod(x + 2, NX)
    yn, yp, yo = mod(y + 1, NY), mod(y + 3, NY), mod(y + 2, NY)
    after, before = mod(s + 1, nseq), mod(s + nseq - 1, nseq)

    loads = {}
    for number, (name, src, dst) in enumerate(
        (("inw", inw_hbm, inw), ("outw", outw_hbm, outw), ("mi", mi_hbm, mi), ("mo", mo_hbm, wsrc.at[2]))
    ):
        loads[name] = pltpu.make_async_copy(src, dst, local_sem.at[number])
    for name in ("mi", "mo", "inw", "outw"):
        loads[name].start()

    barrier = pltpu.get_barrier_semaphore()
    partners = [dev(x_=xn), dev(x_=xp), sibling]
    partners += [(near, mod(t + n, 8)) for near in (after, before) for n in range(8)]
    partners += [dev(y_=mod(y + k, NY)) for k in range(1, NY)]
    partners += [dev(z_=mod(z + k, nz)) for k in range(1, nz)]
    for partner in partners:
        pl.semaphore_signal(barrier, inc=1, device_id=partner, device_id_type=pl.DeviceIdType.MESH)
    pl.semaphore_wait(barrier, len(partners))

    wire = Wire(send_sem, recv_sem)

    def x_piece(i, h):
        return xg.at[i * 2 + c, pl.ds(RIM + h * hm, hm)]

    rims = []
    for n in range(8):
        rims.append(
            wire.message(
                x_ref.at[pl.ds(tm - RIM, RIM)], xg.at[t, pl.ds(0, RIM)], xg.at[mod(t + 8 - n, 8), pl.ds(0, RIM)],
                (after, mod(t + n, 8)),
            )
        )
        rims[-1].start()

    def rim_of(b):
        n = mod(t + 8 - b, 8)
        pltpu.make_async_remote_copy(
            src_ref=x_ref.at[pl.ds(tm - RIM, RIM)],
            dst_ref=xg.at[b, pl.ds(0, RIM)],
            send_sem=send_sem.at[n],
            recv_sem=recv_sem.at[n],
            device_id=(after, t),
            device_id_type=pl.DeviceIdType.MESH,
        ).wait_recv()

    xring = Spread(wire, x_piece, x, along_x, own=lambda h: x_ref.at[pl.ds(h * hm, hm)])
    xring.start()
    to_sib = {}
    for name, i in (("own", x), ("prv", xp), ("nxt", xn), ("opp", xo)):
        src = x_ref if name == "own" else xg.at[i * 2 + c, main]
        to_sib[name] = wire.message(src, xg.at[i * 2 + c, main], xg.at[i * 2 + 1 - c, main], sibling)
    to_sib["own"].start()
    xg[t, main] = x_ref[...]

    loads["mi"].wait()
    for g in range(2):
        wsrc[g] = mi[g].astype(F32).T.astype(BF16)
    loads["mo"].wait()

    zn, zp = mod(z + 1, nz), mod(z + nz - 1, nz)
    steps = nz // 2
    assert steps > 1

    class Weights:
        def __init__(self, first, count):
            self.group = pl.ds(first, count)
            self.over_y, self.up, self.down = [], [[]], [[]]
            for k in range(1, NY):
                j, src_y = mod(y + k, NY), mod(y + NY - k, NY)
                self.over_y.append(
                    wire.message(
                        self.rows(j), self.lanes(0, s * lanes, lanes), self.lanes(0, (z * NY + src_y) * lanes, lanes),
                        along_y(j),
                    )
                )
            for k in range(NY):
                at = mod(y + NY - k, NY) * lanes
                here = self.lanes(0, z * zl + at, lanes)
                src = self.rows(y) if k == 0 else here
                self.up[0].append(wire.message(src, here, self.lanes(0, zp * zl + at, lanes), dev(z_=zn)))
                self.down[0].append(wire.message(src, here, self.lanes(0, zn * zl + at, lanes), dev(z_=zp)))
            self.to_sib = [[self.sib(z * zl, zl)]]
            for k in range(1, steps + 1):
                half = zl // 2 if k == steps else zl
                up, up_in = mod(z + nz - (k - 1), nz) * zl, mod(z + nz - k, nz) * zl
                down, down_in = mod(z + k - 1, nz) * zl + zl - half, mod(z + k, nz) * zl + zl - half
                if k > 1:
                    here, there = self.lanes(0, up, half), self.lanes(0, up_in, half)
                    self.up.append([wire.message(here, here, there, dev(z_=zn))])
                    here, there = self.lanes(0, down, half), self.lanes(0, down_in, half)
                    self.down.append([wire.message(here, here, there, dev(z_=zp))])
                self.to_sib.append([self.sib(up_in, half), self.sib(down_in, half)])

        def rows(self, j):
            return wsrc.at[self.group, pl.ds(pl.multiple_of(j * ff, 16), ff)]

        def lanes(self, slot, start, size):
            return wt.at[self.group, pl.ds(slot * ff, ff), pl.ds(pl.multiple_of(start, 128), size)]

        def sib(self, start, size):
            return wire.message(self.lanes(0, start, size), self.lanes(1, start, size), self.lanes(1, start, size), sibling)

        def split(self):
            for k in (0, 2, 1):
                self.over_y[k].start()

        def first(self, k):
            if k > 0:
                self.over_y[k - 1].arrived()
            self.up[0][k].start()
            self.down[0][k].start()

        def own_to_sib(self):
            self.to_sib[0][0].start()

        def step(self, k):
            for ring, n in ((self.up, 0), (self.down, 1)):
                for message in ring[k - 1]:
                    message.arrived()
                if k < steps:
                    ring[k][0].start()
            for message in self.to_sib[k]:
                message.start()

        def finish(self):
            for messages in self.to_sib:
                for message in messages:
                    message.arrived()

    w_in, w_down = Weights(0, 2), Weights(2, 1)
    w_in.split()
    w_in.first(0)
    w_down.split()
    wt[:, pl.ds(0, ff), pl.ds(pl.multiple_of(s * lanes, 128), lanes)] = wsrc[:, pl.ds(pl.multiple_of(y * ff, 16), ff)]

    acc[...] = jnp.zeros_like(acc)
    ss[...] = jnp.zeros_like(ss)
    loads["inw"].wait()
    order = [t, x * 2 + 1 - c, xp * 2 + c, xn * 2 + c, xp * 2 + 1 - c, xn * 2 + 1 - c, xo * 2 + c, xo * 2 + 1 - c]

    def step_2():
        xring.forward()
        xring.prv_done()
        to_sib["prv"].start()
        w_in.first(1)
        w_in.first(3)

    def step_3():
        xring.nxt_done()
        to_sib["nxt"].start()
        w_in.first(2)

    def step_6():
        xring.opp_done()
        to_sib["opp"].start()
        for k in range(NY):
            w_down.first(k)

    arrivals = {
        1: to_sib["own"].arrived,
        2: step_2,
        3: step_3,
        4: to_sib["prv"].arrived,
        5: to_sib["nxt"].arrived,
        6: step_6,
        7: to_sib["opp"].arrived,
    }

    def take(k, _):
        for at, step in arrivals.items():
            pl.when(k == at)(step)
        b = picked(k, order)
        rim_of(b)
        at = pl.multiple_of(b * cw, 128)
        block = xg[b].astype(F32)
        ss[...] += lane_sums(block * block)
        scaled = (block * ng_ref[:, pl.ds(at, cw)]).astype(BF16)
        for g in range(2):
            acc[g] += jnp.dot(scaled, inw[g, pl.ds(at, cw)], preferred_element_type=F32)
        return 0

    lax.fori_loop(0, 8, take, 0)
    scale = lax.rsqrt(jnp.sum(ss[...], axis=1, keepdims=True) * (1.0 / d) + EPS)
    w_in.own_to_sib()
    w_down.own_to_sib()
    branch_x = (acc[0] * scale).astype(BF16).astype(F32)
    known = jnp.logical_or(s > 0, lax.broadcasted_iota(jnp.int32, branch_x.shape, 0) >= RIM)
    branch_x = jnp.where(known, branch_x, 0.0)
    acc[1] = jax.nn.gelu(acc[1] * scale, approximate=True)

    convolved = jnp.zeros((tm, ch), F32) + cb_ref[...]
    for k in range(cw_ref.shape[0]):
        convolved = convolved + cw_ref[k : k + 1] * pltpu.roll(branch_x, k, 0)[RIM:]
    conv_out = convolved.astype(BF16)
    gates = [
        jnp.dot(conv_out, gw_ref[g, 0], preferred_element_type=F32) + gb_ref[g : g + 1] for g in range(2)
    ]
    log_decay = -8.0 * jax.nn.sigmoid(gates[0]) * dr_ref[...]
    decay = jnp.exp(log_decay)
    driven = conv_out.astype(F32) * jax.nn.sigmoid(gates[1]) * jnp.sqrt(expm1_negated(2.0 * log_decay))
    row = lax.broadcasted_iota(jnp.int32, (tm, ch), 0)
    step = 1
    while step < tm:
        inside = row >= step
        driven = driven + decay * jnp.where(inside, pltpu.roll(driven, step, 0), 0.0)
        decay = decay * jnp.where(inside, pltpu.roll(decay, step, 0), 1.0)
        step *= 2
    ytab[y, 0:1] = decay[tm - 1 :]
    ytab[y, 1:2] = driven[tm - 1 :]
    over_y = []
    for k in range(1, NY):
        over_y.append(
            wire.message(ytab.at[y], ytab.at[y], ytab.at[mod(y + NY - k, NY)], along_y(mod(y + k, NY)))
        )
        over_y[-1].start()
    for message in over_y:
        message.arrived()
    total_a, total_b = jnp.ones((1, ch), F32), jnp.zeros((1, ch), F32)
    before_a, before_b = total_a, total_b
    for j in range(NY):
        a, b = ytab[j, 0:1], ytab[j, 1:2]
        before_b = jnp.where(j < y, a * before_b + b, before_b)
        before_a = jnp.where(j < y, a * before_a, before_a)
        total_b = a * total_b + b
        total_a = a * total_a
    ztab[z, 0:1] = total_a
    ztab[z, 1:2] = total_b
    over_z = []
    for k in range(1, nz):
        over_z.append(
            wire.message(ztab.at[z], ztab.at[z], ztab.at[mod(z + nz - k, nz)], dev(z_=mod(z + k, nz)))
        )
        over_z[-1].start()
    for message in over_z:
        message.arrived()
    carry = jnp.zeros((1, ch), F32)
    for j in range(nz):
        carry = jnp.where(j < z, ztab[j, 0:1] * carry + ztab[j, 1:2], carry)
    carry = before_a * carry + before_b
    mixed[...] = ((decay * carry + driven) * acc[1, RIM:]).astype(BF16)
    w_in.step(1)
    w_down.step(1)

    loads["outw"].wait()
    columns = (xo, xn, xp, x)

    def block(i):
        return pl.ds(pl.multiple_of(i * cw, 128), cw)

    over_d2d = []
    for n, i in enumerate(columns):
        for core in (1 - c, c):
            at = pl.multiple_of((i * 2 + core) * cw, 128)
            part = jnp.dot(mixed[...], outw[:, pl.ds(at, cw)], preferred_element_type=F32)
            op[core, :, block(i)] = part.astype(BF16)
            if core is not c:
                over_d2d.append(wire.message(op.at[1 - c, :, block(i)], oi.at[n], oi.at[n], sibling))
                over_d2d[-1].start()

    out_ring = Gathered(wire, lambda i, h: op.at[c, pl.ds(h * hm, hm), block(i)], x, along_x, obox)
    starts = (out_ring.start_far, out_ring.start_next, out_ring.start_prev, lambda: None)
    for n, i in enumerate(columns):
        over_d2d[n].arrived()
        op[c, :, block(i)] = (op[c, :, block(i)].astype(F32) + oi[n].astype(F32)).astype(BF16)
        starts[n]()
    out_ring.relay()
    for h, value in enumerate(out_ring.result()):
        rows = pl.ds(h * hm, hm)
        res[rows] = (x_ref[rows].astype(F32) + value).astype(BF16)

    def token(j, h=None):
        if h is None:
            return pl.ds(pl.multiple_of(j * rm, 16), rm)
        return pl.ds(pl.multiple_of(j * rm + h * (rm // 2), 16), rm // 2)

    mine, theirs = pl.ds(pl.multiple_of(c * rm, 16), rm), pl.ds(pl.multiple_of((1 - c) * rm, 16), rm)
    swap = wire.message(
        res.at[theirs], xt.at[c, token(y), block(x)], xt.at[1 - c, token(y), block(x)], sibling,
    )
    swap.start()
    xt[c, token(y), block(x)] = res[mine]
    other = 1 - c
    a_x = Spread(wire, lambda i, h: xt.at[c, token(y, h), block(i)], x, along_x)
    a_y = [
        Spread(wire, lambda j, h, i=i: xt.at[c, token(j, h), block(i)], y, along_y) for i in (x, xp, xn, xo)
    ]
    b_y = Spread(wire, lambda j, h: xt.at[other, token(j, h), block(x)], y, along_y)
    b_x = [
        Spread(wire, lambda i, h, j=j: xt.at[other, token(j, h), block(i)], x, along_x) for j in (y, yp, yn, yo)
    ]
    a_x.start()
    swap.arrived()
    b_y.start()
    a_y[0].start()
    b_x[0].start()
    for k in range(2, min(3, steps)):
        w_in.step(k)
        w_down.step(k)
    a_x.forward()
    b_y.forward()
    a_x.prv_done()
    a_y[1].start()
    b_y.prv_done()
    b_x[1].start()
    a_x.nxt_done()
    a_y[2].start()
    b_y.nxt_done()
    b_x[2].start()
    for k in range(3, steps):
        w_in.step(k)
        w_down.step(k)
    a_y[0].forward()
    b_x[0].forward()
    a_x.opp_done()
    a_y[3].start()
    b_y.opp_done()
    b_x[3].start()
    acc2[...] = jnp.zeros_like(acc2)
    ss2[...] = jnp.zeros_like(ss2)

    def ring_done(ring):
        ring.prv_done()
        ring.nxt_done()
        ring.opp_done()

    def rows_0():
        a_y[1].forward()
        b_x[1].forward()
        ring_done(a_y[0])
        w_in.step(steps)
        w_in.finish()

    def rows_1():
        a_y[2].forward()
        b_x[2].forward()

    def rows_2():
        a_y[3].forward()
        b_x[3].forward()
        ring_done(a_y[1])

    def rows_3():
        ring_done(a_y[2])

    def rows_4():
        for ring in b_x:
            ring.prv_done()

    def rows_5():
        for ring in b_x:
            ring.nxt_done()

    def rows_6():
        ring_done(a_y[3])

    def rows_7():
        for ring in b_x:
            ring.opp_done()

    row_steps = (rows_0, rows_1, rows_2, rows_3, rows_4, rows_5, rows_6, rows_7)
    which = ((c, x), (other, x), (c, xp), (c, xn), (other, xp), (other, xn), (c, xo), (other, xo))

    def multiply(k, _):
        for at, step in enumerate(row_steps):
            pl.when(k == at)(step)
        core, i = picked(k, [w[0] for w in which]), picked(k, [w[1] for w in which])
        at = pl.multiple_of((i * 2 + core) * cw, 128)
        rows = xt[core, :, block(i)].astype(F32)
        ss2[...] += lane_sums(rows * rows)
        scaled = (rows * mg_ref[:, pl.ds(at, cw)]).astype(BF16)
        for g in range(2):
            acc2[g] += lax.dot_general(
                scaled, wt[g, :, pl.ds(at, cw)], (((1,), (1,)), ((), ())), preferred_element_type=F32
            )
        return 0

    lax.fori_loop(0, 8, multiply, 0)
    w_down.step(steps)
    w_down.finish()
    scale2 = lax.rsqrt(jnp.sum(ss2[...], axis=1, keepdims=True) * (1.0 / d) + EPS)
    hid[...] = (jax.nn.gelu(acc2[0] * scale2, approximate=True) * (acc2[1] * scale2)).astype(BF16)

    a_back = [
        Gathered(wire, lambda j, h, i=i: po.at[c, token(j, h), block(i)], y, along_y, abox.at[n])
        for n, i in enumerate(columns)
    ]
    b_rows = (yo, yn, yp, y)
    b_back = [
        Gathered(wire, lambda i, h, j=j: po.at[other, token(j, h), block(i)], x, along_x, bbox.at[n])
        for n, j in enumerate(b_rows)
    ]
    a_last = Gathered(wire, lambda i, h: po.at[c, token(y, h), block(i)], x, along_x, abox2)
    b_last = Gathered(wire, lambda j, h: po.at[other, token(j, h), block(x)], y, along_y, bbox2)

    def down_block(core, i):
        at = pl.multiple_of((i * 2 + core) * cw, 128)
        part = jnp.dot(hid[...], wt[2, :, pl.ds(at, cw)], preferred_element_type=F32)
        po[core, :, block(i)] = part.astype(BF16)

    def a_all(n):
        a_back[n].start_far()
        a_back[n].start_next()
        a_back[n].start_prev()

    def b_all(method):
        for ring in b_back:
            getattr(ring, method)()

    down_steps = {
        0: lambda: a_all(0),
        1: lambda: b_all("start_far"),
        2: lambda: a_all(1),
        3: lambda: b_all("start_next"),
        4: lambda: a_all(2),
        5: lambda: b_all("start_prev"),
        6: lambda: a_all(3),
    }

    def down(k, _):
        down_block(picked(lax.rem(k, 2), [c, other]), picked(lax.div(k, 2), list(columns)))
        for at, step in down_steps.items():
            pl.when(k == at)(step)
        return 0

    lax.fori_loop(0, 8, down, 0)

    a_starts = (a_last.start_far, a_last.start_next, a_last.start_prev, lambda: None)
    b_starts = (b_last.start_far, b_last.start_next, b_last.start_prev, lambda: None)
    for n in range(4):
        a_back[n].relay()
        b_back[n].relay()
    for n in range(4):
        for ring, start, core, rows_at, i in (
            (a_back[n], a_starts[n], c, y, columns[n]),
            (b_back[n], b_starts[n], other, b_rows[n], x),
        ):
            for h, value in enumerate(ring.result()):
                po[core, token(rows_at, h), block(i)] = value.astype(BF16)
            start()
    b_last.relay()
    a_last.relay()
    for h, value in enumerate(b_last.result()):
        give[pl.ds(h * (rm // 2), rm // 2)] = value.astype(BF16)
    back = wire.message(give, got, got, sibling)
    back.start()
    for h, value in enumerate(a_last.result()):
        rows = pl.ds(pl.multiple_of(c * rm + h * (rm // 2), 16), rm // 2)
        o_ref[rows] = (res[rows].astype(F32) + value).astype(BF16)
    back.arrived()
    o_ref[theirs] = (res[theirs].astype(F32) + got[...].astype(F32)).astype(BF16)
    wire.drain()


def shards(
    nz, layer_input, norm_gain, in_weights, conv_weight, conv_bias, gate_weights, gate_bias, decay_rate, out_weight,
    mlp_gain, mlp_in, mlp_out,
):
    tm, cw = layer_input.shape
    d, ch = in_weights.shape[1:]
    units = mlp_out.shape[0]
    ff = units // NY
    rm = tm // 2
    vmem = pl.BlockSpec(memory_space=pltpu.VMEM)
    hbm = pl.BlockSpec(memory_space=pl.ANY)
    scratch = [
        ((8, RIM + tm, cw), BF16),
        ((2, d, ch), BF16),
        ((ch, d), BF16),
        (mlp_in.shape, BF16),
        ((3, units, mlp_in.shape[1]), BF16),
        ((3, 2 * ff, d), BF16),
        ((2, RIM + tm, ch), F32),
        ((RIM + tm, 128), F32),
        ((NY, 2, ch), F32),
        ((nz, 2, ch), F32),
        ((tm, ch), BF16),
        ((2, tm, NX * cw), BF16),
        ((4, tm, cw), BF16),
        ((6, tm // 2, cw), BF16),
        ((tm, cw), BF16),
        ((2, NY * rm, NX * cw), BF16),
        ((2, NY * rm, 2 * ff), F32),
        ((NY * rm, 128), F32),
        ((NY * rm, 2 * ff), BF16),
        ((2, NY * rm, NX * cw), BF16),
        ((4, 6, rm // 2, cw), BF16),
        ((4, 6, rm // 2, cw), BF16),
        ((6, rm // 2, cw), BF16),
        ((6, rm // 2, cw), BF16),
        ((rm, cw), BF16),
        ((rm, cw), BF16),
    ]
    call = pl.pallas_call(
        functools.partial(kernel, nz),
        out_shape=jax.ShapeDtypeStruct((tm, cw), BF16),
        in_specs=[vmem] * 8 + [hbm] * 4,
        out_specs=vmem,
        scratch_shapes=[pltpu.VMEM(shape, dtype) for shape, dtype in scratch]
        + [
            pltpu.SemaphoreType.DMA((MESSAGES,)),
            pltpu.SemaphoreType.DMA((MESSAGES,)),
            pltpu.SemaphoreType.DMA((4,)),
        ],
        compiler_params=pltpu.CompilerParams(
            collective_id=0, has_side_effects=True, vmem_limit_bytes=56 * 1024 * 1024
        ),
    )
    return call(
        layer_input, norm_gain[None], conv_weight, conv_bias[None], gate_weights, gate_bias, decay_rate[None],
        mlp_gain[None], in_weights, out_weight, mlp_in, mlp_out,
    )


def solution(mesh):
    return jax.shard_map(
        functools.partial(shards, mesh.shape["seq"] // NY),
        mesh=mesh,
        in_specs=(
            P("seq", "tensor"),
            P(),
            P(None, None, "tensor"),
            P(None, "tensor"),
            P("tensor"),
            P(None, "tensor", None, None),
            P(None, "tensor"),
            P("tensor"),
            P("tensor", None),
            P(),
            P(None, "seq", "tensor"),
            P("tensor", "seq"),
        ),
        out_specs=P("seq", "tensor"),
        check_vma=False,
    )
```

```python
import functools

import jax
import jax.numpy as jnp
from jax import lax
from jax.experimental import pallas as pl
from jax.experimental.pallas import tpu as pltpu
from jax.sharding import PartitionSpec as P

NY = 4
NX = 4
EPS = 1e-06
F32 = jnp.float32
BF16 = jnp.bfloat16
MESSAGES = 352
RIM = 8
GROUPS = 2


def mod(value, size):
    return lax.rem(value + size, size)


def expm1_negated(v):
    series = 1.0 + v * (1.0 / 9.0)
    for n in range(8, 1, -1):
        series = 1.0 + v * (1.0 / n) * series
    return jnp.where(v > -0.5, -v * series, 1.0 - jnp.exp(v))


class Wire:
    def __init__(self, send, recv):
        self.send, self.recv, self.used, self.lots = send, recv, 0, []

    def lot(self, whole):
        self.lots.append(whole)
        return Lot(self, len(self.lots) - 1)

    def drain(self):
        for number, whole in enumerate(self.lots):
            pltpu.make_async_copy(whole, whole, self.send.at[number]).wait()


class Lot:
    def __init__(self, wire, number):
        self.wire, self.number = wire, number

    def message(self, src, dst, landing, device):
        self.wire.used += 1
        return Message(self.wire.send.at[self.number], self.wire.recv.at[self.wire.used - 1], src, dst, landing, device)


class Message:
    def __init__(self, send, recv, src, dst, landing, device):
        self.send, self.recv, self.src, self.dst, self.landing, self.device = send, recv, src, dst, landing, device

    def copy(self, dst):
        return pltpu.make_async_remote_copy(
            src_ref=self.src,
            dst_ref=dst,
            send_sem=self.send,
            recv_sem=self.recv,
            device_id=self.device,
            device_id_type=pl.DeviceIdType.MESH,
        )

    def start(self):
        self.copy(self.dst).start()

    def arrived(self):
        self.copy(self.landing).wait_recv()


class Spread:
    def __init__(self, lot, piece, me, device_of, own=None):
        nxt, prv, opp = mod(me + 1, 4), mod(me + 3, 4), mod(me + 2, 4)
        own = own or (lambda h: piece(me, h))
        self.na = lot.message(own(0), piece(me, 0), piece(prv, 0), device_of(nxt))
        self.nb = lot.message(own(1), piece(me, 1), piece(prv, 1), device_of(nxt))
        self.pb = lot.message(own(1), piece(me, 1), piece(nxt, 1), device_of(prv))
        self.pa = lot.message(own(0), piece(me, 0), piece(nxt, 0), device_of(prv))
        self.fn = lot.message(piece(prv, 0), piece(prv, 0), piece(opp, 0), device_of(nxt))
        self.fp = lot.message(piece(nxt, 1), piece(nxt, 1), piece(opp, 1), device_of(prv))

    def start(self):
        self.na.start()
        self.pb.start()
        self.nb.start()
        self.pa.start()

    def forward(self):
        self.na.arrived()
        self.fn.start()
        self.pb.arrived()
        self.fp.start()

    def prv_done(self):
        self.nb.arrived()

    def nxt_done(self):
        self.pa.arrived()

    def opp_done(self):
        self.fn.arrived()
        self.fp.arrived()


class Gathered:
    def __init__(self, lot, part, me, device_of, box):
        nxt, prv, opp = mod(me + 1, 4), mod(me + 3, 4), mod(me + 2, 4)
        self.part, self.me, self.nxt, self.prv, self.box = part, me, nxt, prv, box
        def send(src, slot, device):
            return lot.message(src, box.at[slot], box.at[slot], device)
        self.oa = send(part(opp, 0), 0, device_of(nxt))
        self.ob = send(part(opp, 1), 1, device_of(prv))
        self.db = send(part(nxt, 1), 2, device_of(nxt))
        self.da = send(part(prv, 0), 3, device_of(prv))
        self.ca = send(part(nxt, 0), 4, device_of(nxt))
        self.cb = send(part(prv, 1), 5, device_of(prv))

    def start_far(self):
        self.oa.start()
        self.ob.start()

    def start_next(self):
        self.db.start()

    def start_prev(self):
        self.da.start()

    def relay(self):
        for arriving, leaving, member, half, slot in (
            (self.oa, self.ca, self.nxt, 0, 0),
            (self.ob, self.cb, self.prv, 1, 1),
        ):
            arriving.arrived()
            ref = self.part(member, half)
            ref[...] = (ref[...].astype(F32) + self.box[slot].astype(F32)).astype(BF16)
            leaving.start()

    def result(self):
        self.da.arrived()
        self.ca.arrived()
        self.db.arrived()
        self.cb.arrived()
        halves = []
        for half, slots in ((0, (4, 3)), (1, (2, 5))):
            value = self.part(self.me, half)[...].astype(F32)
            for slot in slots:
                value = value + self.box[slot].astype(F32)
            halves.append(value)
        return halves


def lane_sums(value):
    return sum(value[:, at : at + 128] for at in range(128, value.shape[1], 128)) + value[:, :128]


def at_step(k, steps):
    for number, step in steps.items():

        def run(step=step):
            step()

        pl.when(k == number)(run)


def picked(k, values):
    result = values[0]
    for n in range(1, len(values)):
        result = jnp.where(k == n, values[n], result)
    return result


def kernel(
    nz, x_ref, ng_ref, cw_ref, cb_ref, gw_ref, gb_ref, dr_ref, mg_ref, inw_hbm, outw_hbm, mi_hbm, mo_hbm, o_ref,
    xg, inw, outw, mi, wsrc, wt, acc, ss, ytab, ztab, mixed, op, oi, obox, res,
    xt, acc2, ss2, hid, po, abox, bbox, abox2, bbox2, give, got, send_sem, recv_sem, local_sem,
):
    tm, cw = x_ref.shape
    hm = tm // 2
    ch = gw_ref.shape[2]
    d = ng_ref.shape[1]
    rm = tm // 2
    ff = wsrc.shape[1] // NY
    lanes = d // (nz * NY)
    zl = NY * lanes
    nseq = nz * NY
    main = pl.ds(RIM, tm)

    s = lax.axis_index("seq")
    t = lax.axis_index("tensor")
    z, y = lax.div(s, NY), lax.rem(s, NY)
    x, c = lax.div(t, 2), lax.rem(t, 2)

    def dev(z_=None, y_=None, x_=None, c_=None):
        z_, y_ = (z if z_ is None else z_), (y if y_ is None else y_)
        x_, c_ = (x if x_ is None else x_), (c if c_ is None else c_)
        return (z_ * NY + y_, x_ * 2 + c_)

    along_x = lambda i: dev(x_=i)
    along_y = lambda j: dev(y_=j)
    sibling = dev(c_=1 - c)
    xn, xp, xo = mod(x + 1, NX), mod(x + 3, NX), mod(x + 2, NX)
    yn, yp, yo = mod(y + 1, NY), mod(y + 3, NY), mod(y + 2, NY)
    after, before = mod(s + 1, nseq), mod(s + nseq - 1, nseq)

    loads = {}
    for number, (name, src, dst) in enumerate(
        (("inw", inw_hbm, inw), ("outw", outw_hbm, outw), ("mi", mi_hbm, mi), ("mo", mo_hbm, wsrc.at[2]))
    ):
        loads[name] = pltpu.make_async_copy(src, dst, local_sem.at[number])
    for name in ("mi", "mo", "inw", "outw"):
        loads[name].start()

    barrier = pltpu.get_barrier_semaphore()
    partners = [dev(x_=xn), dev(x_=xp), sibling]
    partners += [(near, mod(t + n, 8)) for near in (after, before) for n in range(8)]
    partners += [dev(y_=mod(y + k, NY)) for k in range(1, NY)]
    partners += [dev(z_=mod(z + k, nz)) for k in range(1, nz)]
    for partner in partners:
        pl.semaphore_signal(barrier, inc=1, device_id=partner, device_id_type=pl.DeviceIdType.MESH)
    pl.semaphore_wait(barrier, len(partners))

    wire = Wire(send_sem, recv_sem)

    def x_piece(i, h):
        return xg.at[i * 2 + c, pl.ds(RIM + h * hm, hm)]

    lot = wire.lot(xg.at[0, pl.ds(0, 8 * RIM)])
    rims = []
    for n in range(8):
        rims.append(
            lot.message(
                x_ref.at[pl.ds(tm - RIM, RIM)], xg.at[t, pl.ds(0, RIM)], xg.at[mod(t + 8 - n, 8), pl.ds(0, RIM)],
                (after, mod(t + n, 8)),
            )
        )
        rims[-1].start()

    def rim_of(b):
        n = mod(t + 8 - b, 8)
        pltpu.make_async_remote_copy(
            src_ref=x_ref.at[pl.ds(tm - RIM, RIM)],
            dst_ref=xg.at[b, pl.ds(0, RIM)],
            send_sem=send_sem.at[0],
            recv_sem=recv_sem.at[n],
            device_id=(after, t),
            device_id_type=pl.DeviceIdType.MESH,
        ).wait_recv()

    xring = Spread(wire.lot(obox), x_piece, x, along_x, own=lambda h: x_ref.at[pl.ds(h * hm, hm)])
    xring.start()
    to_sib = {}
    lot = wire.lot(oi)
    for name, i in (("own", x), ("prv", xp), ("nxt", xn), ("opp", xo)):
        src = x_ref if name == "own" else xg.at[i * 2 + c, main]
        to_sib[name] = lot.message(src, xg.at[i * 2 + c, main], xg.at[i * 2 + 1 - c, main], sibling)
    to_sib["own"].start()
    xg[t, main] = x_ref[...]

    loads["mi"].wait()
    for g in range(2):
        wsrc[g] = mi[g].astype(F32).T.astype(BF16)
    loads["mo"].wait()

    zn, zp = mod(z + 1, nz), mod(z + nz - 1, nz)
    steps = nz // 2
    assert steps > 1

    class Weights:
        def __init__(self, first, count):
            self.group = pl.ds(first, count)
            self.over_y, self.up, self.down = [], [[]], [[]]
            self.ring = wire.lot(self.lanes(0, 0, (3 * NY - 1) * lanes + (nz - 1) * zl - 2 * zl))
            self.pair = wire.lot(self.lanes(0, 0, d))
            for k in range(1, NY):
                j, src_y = mod(y + k, NY), mod(y + NY - k, NY)
                self.over_y.append(
                    self.ring.message(
                        self.rows(j), self.lanes(0, s * lanes, lanes), self.lanes(0, (z * NY + src_y) * lanes, lanes),
                        along_y(j),
                    )
                )
            for k in range(NY):
                at = mod(y + NY - k, NY) * lanes
                here = self.lanes(0, z * zl + at, lanes)
                src = self.rows(y) if k == 0 else here
                self.up[0].append(self.ring.message(src, here, self.lanes(0, zp * zl + at, lanes), dev(z_=zn)))
                self.down[0].append(self.ring.message(src, here, self.lanes(0, zn * zl + at, lanes), dev(z_=zp)))
            self.to_sib = [[self.sib(z * zl, zl)]]
            for k in range(1, steps + 1):
                half = zl // 2 if k == steps else zl
                up, up_in = mod(z + nz - (k - 1), nz) * zl, mod(z + nz - k, nz) * zl
                down, down_in = mod(z + k - 1, nz) * zl + zl - half, mod(z + k, nz) * zl + zl - half
                if k > 1:
                    here, there = self.lanes(0, up, half), self.lanes(0, up_in, half)
                    self.up.append([self.ring.message(here, here, there, dev(z_=zn))])
                    here, there = self.lanes(0, down, half), self.lanes(0, down_in, half)
                    self.down.append([self.ring.message(here, here, there, dev(z_=zp))])
                self.to_sib.append([self.sib(up_in, half), self.sib(down_in, half)])

        def rows(self, j):
            return wsrc.at[self.group, pl.ds(pl.multiple_of(j * ff, 16), ff)]

        def lanes(self, slot, start, size):
            return wt.at[self.group, pl.ds(slot * ff, ff), pl.ds(pl.multiple_of(start, 128), size)]

        def sib(self, start, size):
            return self.pair.message(self.lanes(0, start, size), self.lanes(1, start, size), self.lanes(1, start, size), sibling)

        def split(self):
            for k in (0, 2, 1):
                self.over_y[k].start()

        def first(self, k):
            if k > 0:
                self.over_y[k - 1].arrived()
            self.up[0][k].start()
            self.down[0][k].start()

        def own_to_sib(self):
            self.to_sib[0][0].start()

        def step(self, k):
            for ring, n in ((self.up, 0), (self.down, 1)):
                for message in ring[k - 1]:
                    message.arrived()
                if k < steps:
                    ring[k][0].start()
            for message in self.to_sib[k]:
                message.start()

        def finish(self):
            for messages in self.to_sib:
                for message in messages:
                    message.arrived()

    w_in, w_down = Weights(0, 2), Weights(2, 1)
    w_in.split()
    w_in.first(0)
    w_down.split()
    wt[:, pl.ds(0, ff), pl.ds(pl.multiple_of(s * lanes, 128), lanes)] = wsrc[:, pl.ds(pl.multiple_of(y * ff, 16), ff)]

    acc[...] = jnp.zeros_like(acc)
    ss[...] = jnp.zeros_like(ss)
    loads["inw"].wait()
    order = [t, x * 2 + 1 - c, xp * 2 + c, xn * 2 + c, xp * 2 + 1 - c, xn * 2 + 1 - c, xo * 2 + c, xo * 2 + 1 - c]

    def step_2():
        xring.forward()
        xring.prv_done()
        to_sib["prv"].start()
        w_in.first(1)
        w_in.first(3)

    def step_3():
        xring.nxt_done()
        to_sib["nxt"].start()
        w_in.first(2)

    def step_6():
        xring.opp_done()
        to_sib["opp"].start()
        for k in range(NY):
            w_down.first(k)

    arrivals = {
        1: to_sib["own"].arrived,
        2: step_2,
        3: step_3,
        4: to_sib["prv"].arrived,
        5: to_sib["nxt"].arrived,
        6: step_6,
        7: to_sib["opp"].arrived,
    }

    def take(k, _):
        at_step(k, arrivals)
        b = picked(k, order)
        rim_of(b)
        at = pl.multiple_of(b * cw, 128)
        block = xg[b].astype(F32)
        ss[...] += lane_sums(block * block)
        scaled = (block * ng_ref[:, pl.ds(at, cw)]).astype(BF16)
        for g in range(2):
            acc[g] += jnp.dot(scaled, inw[g, pl.ds(at, cw)], preferred_element_type=F32)
        return 0

    lax.fori_loop(0, 8, take, 0)
    scale = lax.rsqrt(jnp.sum(ss[...], axis=1, keepdims=True) * (1.0 / d) + EPS)
    w_in.own_to_sib()
    w_down.own_to_sib()
    branch_x = (acc[0] * scale).astype(BF16).astype(F32)
    known = jnp.logical_or(s > 0, lax.broadcasted_iota(jnp.int32, branch_x.shape, 0) >= RIM)
    branch_x = jnp.where(known, branch_x, 0.0)
    acc[1] = jax.nn.gelu(acc[1] * scale, approximate=True)

    convolved = jnp.zeros((tm, ch), F32) + cb_ref[...]
    for k in range(cw_ref.shape[0]):
        convolved = convolved + cw_ref[k : k + 1] * pltpu.roll(branch_x, k, 0)[RIM:]
    conv_out = convolved.astype(BF16)
    gates = [
        jnp.dot(conv_out, gw_ref[g, 0], preferred_element_type=F32) + gb_ref[g : g + 1] for g in range(2)
    ]
    log_decay = -8.0 * jax.nn.sigmoid(gates[0]) * dr_ref[...]
    decay = jnp.exp(log_decay)
    driven = conv_out.astype(F32) * jax.nn.sigmoid(gates[1]) * jnp.sqrt(expm1_negated(2.0 * log_decay))
    row = lax.broadcasted_iota(jnp.int32, (tm, ch), 0)
    step = 1
    while step < tm:
        inside = row >= step
        driven = driven + decay * jnp.where(inside, pltpu.roll(driven, step, 0), 0.0)
        decay = decay * jnp.where(inside, pltpu.roll(decay, step, 0), 1.0)
        step *= 2
    ytab[y, 0:1] = decay[tm - 1 :]
    ytab[y, 1:2] = driven[tm - 1 :]
    over_y = []
    lot = wire.lot(ytab.at[pl.ds(0, NY - 1)])
    for k in range(1, NY):
        over_y.append(
            lot.message(ytab.at[y], ytab.at[y], ytab.at[mod(y + NY - k, NY)], along_y(mod(y + k, NY)))
        )
        over_y[-1].start()
    for message in over_y:
        message.arrived()
    total_a, total_b = jnp.ones((1, ch), F32), jnp.zeros((1, ch), F32)
    before_a, before_b = total_a, total_b
    for j in range(NY):
        a, b = ytab[j, 0:1], ytab[j, 1:2]
        before_b = jnp.where(j < y, a * before_b + b, before_b)
        before_a = jnp.where(j < y, a * before_a, before_a)
        total_b = a * total_b + b
        total_a = a * total_a
    ztab[z, 0:1] = total_a
    ztab[z, 1:2] = total_b
    over_z = []
    lot = wire.lot(ztab.at[pl.ds(0, nz - 1)])
    for k in range(1, nz):
        over_z.append(
            lot.message(ztab.at[z], ztab.at[z], ztab.at[mod(z + nz - k, nz)], dev(z_=mod(z + k, nz)))
        )
        over_z[-1].start()
    for message in over_z:
        message.arrived()
    carry = jnp.zeros((1, ch), F32)
    for j in range(nz):
        carry = jnp.where(j < z, ztab[j, 0:1] * carry + ztab[j, 1:2], carry)
    carry = before_a * carry + before_b
    mixed[...] = ((decay * carry + driven) * acc[1, RIM:]).astype(BF16)
    w_in.step(1)
    w_down.step(1)

    loads["outw"].wait()
    columns = (xo, xn, xp, x)

    def block(i):
        return pl.ds(pl.multiple_of(i * cw, 128), cw)

    over_d2d = []
    lot = wire.lot(oi)
    for n, i in enumerate(columns):
        for core in (1 - c, c):
            at = pl.multiple_of((i * 2 + core) * cw, 128)
            part = jnp.dot(mixed[...], outw[:, pl.ds(at, cw)], preferred_element_type=F32)
            op[core, :, block(i)] = part.astype(BF16)
            if core is not c:
                over_d2d.append(lot.message(op.at[1 - c, :, block(i)], oi.at[n], oi.at[n], sibling))
                over_d2d[-1].start()

    out_ring = Gathered(wire.lot(obox), lambda i, h: op.at[c, pl.ds(h * hm, hm), block(i)], x, along_x, obox)
    starts = (out_ring.start_far, out_ring.start_next, out_ring.start_prev, lambda: None)
    for n, i in enumerate(columns):
        over_d2d[n].arrived()
        op[c, :, block(i)] = (op[c, :, block(i)].astype(F32) + oi[n].astype(F32)).astype(BF16)
        starts[n]()
    out_ring.relay()
    if steps > 2:
        w_in.step(2)
    for h, value in enumerate(out_ring.result()):
        rows = pl.ds(h * hm, hm)
        res[rows] = (x_ref[rows].astype(F32) + value).astype(BF16)

    hg = rm // GROUPS
    hh = hg // 2
    other = 1 - c

    def token(j, h):
        return pl.ds(pl.multiple_of(j * hg + h * hh, 16), hh)

    def of_core(core, g, size, h=0):
        return pl.ds(pl.multiple_of(core * rm + g * hg + h * hh, 16), size)

    here_rows = pl.ds(pl.multiple_of(y * hg, 16), hg)

    class Rows:
        def __init__(self, g):
            self.g = g
            there = xt.at[1 - c, g, here_rows, block(x)]
            lot = wire.lot(xt.at[0, :, pl.ds(0, 60 * hh // (NX * GROUPS))])
            self.swap = wire.lot(there).message(res.at[of_core(other, g, hg)], xt.at[c, g, here_rows, block(x)], there, sibling)
            self.a_x = Spread(lot, lambda i, h: xt.at[c, g, token(y, h), block(i)], x, along_x)
            self.a_y = [
                Spread(lot, lambda j, h, i=i: xt.at[c, g, token(j, h), block(i)], y, along_y)
                for i in (x, xp, xn, xo)
            ]
            self.b_y = Spread(lot, lambda j, h: xt.at[other, g, token(j, h), block(x)], y, along_y)
            self.b_x = [
                Spread(lot, lambda i, h, j=j: xt.at[other, g, token(j, h), block(i)], x, along_x)
                for j in (y, yp, yn, yo)
            ]

        def begin(self):
            self.swap.start()
            xt[c, self.g, here_rows, block(x)] = res[of_core(c, self.g, hg)]
            self.a_x.start()

        def begin_other(self):
            self.swap.arrived()
            self.b_y.start()

        def own(self):
            self.a_y[0].start()
            self.b_x[0].start()

        def relay_first(self):
            self.a_x.forward()
            self.b_y.forward()

        def sides(self):
            self.a_x.prv_done()
            self.a_y[1].start()
            self.b_y.prv_done()
            self.b_x[1].start()
            self.a_x.nxt_done()
            self.a_y[2].start()
            self.b_y.nxt_done()
            self.b_x[2].start()

        def far(self):
            self.a_x.opp_done()
            self.a_y[3].start()
            self.b_y.opp_done()
            self.b_x[3].start()

        def relay(self, n):
            self.a_y[n].forward()
            self.b_x[n].forward()

        def a_done(self, n):
            self.a_y[n].prv_done()
            self.a_y[n].nxt_done()
            self.a_y[n].opp_done()

        def b_done(self, which):
            for ring in self.b_x:
                getattr(ring, which)()

    class Sums:
        def __init__(self, g):
            self.g = g
            lot = wire.lot(po.at[0, :, pl.ds(0, 60 * hh // (NX * GROUPS))])
            self.a = [
                Gathered(lot, lambda j, h, i=i: po.at[c, g, token(j, h), block(i)], y, along_y, abox.at[g, n])
                for n, i in enumerate(columns)
            ]
            self.b = [
                Gathered(lot, lambda i, h, j=j: po.at[other, g, token(j, h), block(i)], x, along_x, bbox.at[g, n])
                for n, j in enumerate(b_rows)
            ]
            self.a_last = Gathered(lot, lambda i, h: po.at[c, g, token(y, h), block(i)], x, along_x, abox2.at[g])
            self.b_last = Gathered(lot, lambda j, h: po.at[other, g, token(j, h), block(x)], y, along_y, bbox2.at[g])
            self.back = wire.lot(give.at[g]).message(give.at[g], got.at[g], got.at[g], sibling)

        def a_all(self, n):
            self.a[n].start_far()
            self.a[n].start_next()
            self.a[n].start_prev()

        def b_all(self, method):
            for ring in self.b:
                getattr(ring, method)()

        def down(self):
            starts = (
                lambda: (self.a_all(0), self.b_all("start_far")),
                lambda: (self.a_all(1), self.b_all("start_next")),
                lambda: (self.a_all(2), self.b_all("start_prev")),
                lambda: self.a_all(3),
            )

            def one(k, _):
                i = picked(k, list(columns))
                both = pl.ds(pl.multiple_of(i * 2 * cw, 128), 2 * cw)
                part = jnp.dot(hid[...], wt[2, :, both], preferred_element_type=F32).astype(BF16)
                for core in range(2):
                    po[core, self.g, :, block(i)] = part[:, core * cw : (core + 1) * cw]
                at_step(k, dict(enumerate(starts)))
                return 0

            lax.fori_loop(0, 4, one, 0)

        def relay(self, n):
            self.a[n].relay()
            self.b[n].relay()

        def first_sums(self):
            a_starts = (self.a_last.start_far, self.a_last.start_next, self.a_last.start_prev, lambda: None)
            b_starts = (self.b_last.start_far, self.b_last.start_next, self.b_last.start_prev, lambda: None)
            for n in range(4):
                for ring, start, core, rows_at, i in (
                    (self.a[n], a_starts[n], c, y, columns[n]),
                    (self.b[n], b_starts[n], other, b_rows[n], x),
                ):
                    for h, value in enumerate(ring.result()):
                        po[core, self.g, token(rows_at, h), block(i)] = value.astype(BF16)
                    start()

        def relay_last(self):
            self.b_last.relay()
            self.a_last.relay()

        def results(self):
            for h, value in enumerate(self.b_last.result()):
                give[self.g, pl.ds(h * hh, hh)] = value.astype(BF16)
            self.back.start()
            for h, value in enumerate(self.a_last.result()):
                rows = of_core(c, self.g, hh, h)
                o_ref[rows] = (res[rows].astype(F32) + value).astype(BF16)

        def others(self):
            self.back.arrived()
            rows = of_core(other, self.g, hg)
            o_ref[rows] = (res[rows].astype(F32) + got[self.g].astype(F32)).astype(BF16)

    b_rows = (yo, yn, yp, y)
    rows_0, rows_1 = Rows(0), Rows(1)
    sums_0, sums_1 = Sums(0), Sums(1)

    def multiply(rows, extra):
        pairs = (((c, x), (other, x)), ((c, xp), (c, xn)), ((other, xp), (other, xn)), ((c, xo), (other, xo)))
        waits = {
            0: lambda: rows.a_done(0),
            1: lambda: (rows.a_done(1), rows.a_done(2)),
            2: lambda: (rows.b_done("prv_done"), rows.b_done("nxt_done")),
            3: lambda: (rows.a_done(3), rows.b_done("opp_done")),
        }
        acc2[...] = jnp.zeros_like(acc2)
        ss2[...] = jnp.zeros_like(ss2)

        def one(k, _):
            at_step(k, extra)
            at_step(k, waits)
            scaled, weights, squares = [], [], 0.0
            for n in range(2):
                core, i = picked(k, [w[n][0] for w in pairs]), picked(k, [w[n][1] for w in pairs])
                at = pl.multiple_of((i * 2 + core) * cw, 128)
                block_rows = xt[core, rows.g, :, block(i)].astype(F32)
                squares = squares + lane_sums(block_rows * block_rows)
                scaled.append((block_rows * mg_ref[:, pl.ds(at, cw)]).astype(BF16))
                weights.append(wt[0:2, :, pl.ds(at, cw)].reshape(4 * ff, cw))
            ss2[...] += squares
            acc2[...] += lax.dot_general(
                jnp.concatenate(scaled, axis=1), jnp.concatenate(weights, axis=1), (((1,), (1,)), ((), ())),
                preferred_element_type=F32,
            )
            return 0

        lax.fori_loop(0, 4, one, 0)
        scale2 = lax.rsqrt(jnp.sum(ss2[...], axis=1, keepdims=True) * (1.0 / d) + EPS)
        hid[...] = (jax.nn.gelu(acc2[:, : 2 * ff] * scale2, approximate=True) * (acc2[:, 2 * ff :] * scale2)).astype(BF16)

    rows_0.begin()
    rows_0.begin_other()
    rows_0.own()
    rows_1.begin()
    rows_1.begin_other()
    if steps > 2:
        w_down.step(2)
    rows_0.relay_first()
    rows_0.sides()
    rows_0.relay(0)
    rows_0.far()
    rows_1.relay_first()
    for k in range(3, steps):
        w_in.step(k)
    rows_0.relay(1)
    rows_1.own()
    rows_0.relay(2)
    rows_1.sides()
    rows_0.relay(3)
    rows_1.far()
    w_in.step(steps)
    for k in range(3, steps):
        w_down.step(k)
    w_in.finish()
    multiply(rows_0, {n: functools.partial(rows_1.relay, n) for n in range(4)})
    w_down.step(steps)
    w_down.finish()
    sums_0.down()
    multiply(rows_1, {n: functools.partial(sums_0.relay, n) for n in range(4)})
    sums_1.down()
    sums_0.first_sums()
    for n in range(4):
        sums_1.relay(n)
    sums_0.relay_last()
    sums_1.first_sums()
    sums_0.results()
    sums_1.relay_last()
    sums_0.others()
    sums_1.results()
    sums_1.others()
    wire.drain()


def shards(
    nz, layer_input, norm_gain, in_weights, conv_weight, conv_bias, gate_weights, gate_bias, decay_rate, out_weight,
    mlp_gain, mlp_in, mlp_out,
):
    tm, cw = layer_input.shape
    d, ch = in_weights.shape[1:]
    units = mlp_out.shape[0]
    ff = units // NY
    hg = tm // 2 // GROUPS
    vmem = pl.BlockSpec(memory_space=pltpu.VMEM)
    hbm = pl.BlockSpec(memory_space=pl.ANY)
    scratch = [
        ((8, RIM + tm, cw), BF16),
        ((2, d, ch), BF16),
        ((ch, d), BF16),
        (mlp_in.shape, BF16),
        ((3, units, mlp_in.shape[1]), BF16),
        ((3, 2 * ff, d), BF16),
        ((2, RIM + tm, ch), F32),
        ((RIM + tm, 128), F32),
        ((NY, 2, ch), F32),
        ((nz, 2, ch), F32),
        ((tm, ch), BF16),
        ((2, tm, NX * cw), BF16),
        ((4, tm, cw), BF16),
        ((6, tm // 2, cw), BF16),
        ((tm, cw), BF16),
        ((2, GROUPS, NY * hg, NX * cw), BF16),
        ((NY * hg, 4 * ff), F32),
        ((NY * hg, 128), F32),
        ((NY * hg, 2 * ff), BF16),
        ((2, GROUPS, NY * hg, NX * cw), BF16),
        ((GROUPS, 4, 6, hg // 2, cw), BF16),
        ((GROUPS, 4, 6, hg // 2, cw), BF16),
        ((GROUPS, 6, hg // 2, cw), BF16),
        ((GROUPS, 6, hg // 2, cw), BF16),
        ((GROUPS, hg, cw), BF16),
        ((GROUPS, hg, cw), BF16),
    ]
    call = pl.pallas_call(
        functools.partial(kernel, nz),
        out_shape=jax.ShapeDtypeStruct((tm, cw), BF16),
        in_specs=[vmem] * 8 + [hbm] * 4,
        out_specs=vmem,
        scratch_shapes=[pltpu.VMEM(shape, dtype) for shape, dtype in scratch]
        + [
            pltpu.SemaphoreType.DMA((32,)),
            pltpu.SemaphoreType.DMA((MESSAGES,)),
            pltpu.SemaphoreType.DMA((4,)),
        ],
        compiler_params=pltpu.CompilerParams(
            collective_id=0, has_side_effects=True, vmem_limit_bytes=56 * 1024 * 1024
        ),
    )
    return call(
        layer_input, norm_gain[None], conv_weight, conv_bias[None], gate_weights, gate_bias, decay_rate[None],
        mlp_gain[None], in_weights, out_weight, mlp_in, mlp_out,
    )


def solution(mesh):
    return jax.shard_map(
        functools.partial(shards, mesh.shape["seq"] // NY),
        mesh=mesh,
        in_specs=(
            P("seq", "tensor"),
            P(),
            P(None, None, "tensor"),
            P(None, "tensor"),
            P("tensor"),
            P(None, "tensor", None, None),
            P(None, "tensor"),
            P("tensor"),
            P("tensor", None),
            P(),
            P(None, "seq", "tensor"),
            P("tensor", "seq"),
        ),
        out_specs=P("seq", "tensor"),
        check_vma=False,
    )
```

```python
import functools

import jax
import jax.numpy as jnp
from jax import lax
from jax.experimental import pallas as pl
from jax.experimental.pallas import tpu as pltpu
from jax.sharding import PartitionSpec as P

NY = 4
NX = 4
EPS = 1e-06
F32 = jnp.float32
BF16 = jnp.bfloat16
ARRIVALS = 144
RIM = 8
GROUPS = 2


def mod(value, size):
    return lax.rem(value + size, size)


def expm1_negated(v):
    series = 1.0 + v * (1.0 / 9.0)
    for n in range(8, 1, -1):
        series = 1.0 + v * (1.0 / n) * series
    return jnp.where(v > -0.5, -v * series, 1.0 - jnp.exp(v))


class Wire:
    def __init__(self, send, recv):
        self.send, self.recv, self.used, self.lots = send, recv, 0, []

    def arrival(self):
        self.used += 1
        return self.recv.at[self.used - 1]

    def lot(self, whole):
        self.lots.append(whole)
        return Lot(self, len(self.lots) - 1)

    def drain(self):
        for number, whole in enumerate(self.lots):
            pltpu.make_async_copy(whole, whole, self.send.at[number]).wait()


class Lot:
    def __init__(self, wire, number):
        self.wire, self.number = wire, number

    def message(self, src, dst, landing, device, arrival=None):
        arrival = self.wire.arrival() if arrival is None else arrival
        return Message(self.wire.send.at[self.number], arrival, src, dst, landing, device)


def arrived(semaphore, whole):
    pltpu.make_async_copy(whole, whole, semaphore).wait()


class Message:
    def __init__(self, send, recv, src, dst, landing, device):
        self.send, self.recv, self.src, self.dst, self.landing, self.device = send, recv, src, dst, landing, device

    def copy(self, dst):
        return pltpu.make_async_remote_copy(
            src_ref=self.src,
            dst_ref=dst,
            send_sem=self.send,
            recv_sem=self.recv,
            device_id=self.device,
            device_id_type=pl.DeviceIdType.MESH,
        )

    def start(self):
        self.copy(self.dst).start()

    def arrived(self):
        self.copy(self.landing).wait_recv()


class Spread:
    def __init__(self, lot, piece, me, device_of, own=None):
        nxt, prv, opp = mod(me + 1, 4), mod(me + 3, 4), mod(me + 2, 4)
        own = own or (lambda h: piece(me, h))
        self.na = lot.message(own(0), piece(me, 0), piece(prv, 0), device_of(nxt))
        self.nb = lot.message(own(1), piece(me, 1), piece(prv, 1), device_of(nxt))
        self.pb = lot.message(own(1), piece(me, 1), piece(nxt, 1), device_of(prv))
        self.pa = lot.message(own(0), piece(me, 0), piece(nxt, 0), device_of(prv))
        self.fn = lot.message(piece(prv, 0), piece(prv, 0), piece(opp, 0), device_of(nxt))
        self.fp = lot.message(piece(nxt, 1), piece(nxt, 1), piece(opp, 1), device_of(prv))

    def start(self):
        self.na.start()
        self.pb.start()
        self.nb.start()
        self.pa.start()

    def forward(self):
        self.na.arrived()
        self.fn.start()
        self.pb.arrived()
        self.fp.start()

    def prv_done(self):
        self.nb.arrived()

    def nxt_done(self):
        self.pa.arrived()

    def opp_done(self):
        self.fn.arrived()
        self.fp.arrived()


class Around:
    def __init__(self, lot, piece, part, size, me, device_of, far=None):
        nxt, prv, opp = mod(me + 1, 4), mod(me + 3, 4), mod(me + 2, 4)
        self.near, self.size = lot.wire.arrival(), size
        self.far = lot.wire.arrival() if far is None else far
        self.n = lot.message(part(me), part(me), None, device_of(nxt), self.near)
        self.p = lot.message(part(me), part(me), None, device_of(prv), self.near)
        self.fn = lot.message(piece(prv, 0), piece(prv, 0), None, device_of(nxt), self.far)
        self.fp = lot.message(piece(nxt, 1), piece(nxt, 1), None, device_of(prv), self.far)

    def start(self):
        self.n.start()
        self.p.start()

    def forward(self):
        arrived(self.near, self.size(2))
        self.fn.start()
        self.fp.start()

    def opp_done(self):
        arrived(self.far, self.size(1))


class Gathered:
    def __init__(self, lot, part, me, device_of, box):
        nxt, prv, opp = mod(me + 1, 4), mod(me + 3, 4), mod(me + 2, 4)
        self.part, self.me, self.nxt, self.prv, self.box = part, me, nxt, prv, box
        self.first, self.last = lot.wire.arrival(), lot.wire.arrival()

        def send(src, slot, device):
            return lot.message(src, box.at[slot], None, device, self.first if slot < 2 else self.last)

        self.oa = send(part(opp, 0), 0, device_of(nxt))
        self.ob = send(part(opp, 1), 1, device_of(prv))
        self.db = send(part(nxt, 1), 2, device_of(nxt))
        self.da = send(part(prv, 0), 3, device_of(prv))
        self.ca = send(part(nxt, 0), 4, device_of(nxt))
        self.cb = send(part(prv, 1), 5, device_of(prv))

    def start_far(self):
        self.oa.start()
        self.ob.start()

    def start_next(self):
        self.db.start()

    def start_prev(self):
        self.da.start()

    def relay(self):
        arrived(self.first, self.box.at[pl.ds(0, 2)])
        for leaving, member, half, slot in ((self.ca, self.nxt, 0, 0), (self.cb, self.prv, 1, 1)):
            ref = self.part(member, half)
            ref[...] = (ref[...].astype(F32) + self.box[slot].astype(F32)).astype(BF16)
            leaving.start()

    def result(self):
        arrived(self.last, self.box.at[pl.ds(2, 4)])
        halves = []
        for half, slots in ((0, (4, 3)), (1, (2, 5))):
            value = self.part(self.me, half)[...].astype(F32)
            for slot in slots:
                value = value + self.box[slot].astype(F32)
            halves.append(value)
        return halves


def lane_sums(value):
    return sum(value[:, at : at + 128] for at in range(128, value.shape[1], 128)) + value[:, :128]


def at_step(k, steps):
    for number, step in steps.items():

        def run(step=step):
            step()

        pl.when(k == number)(run)


def picked(k, values):
    result = values[0]
    for n in range(1, len(values)):
        result = jnp.where(k == n, values[n], result)
    return result


def kernel(
    nz, x_ref, ng_ref, cw_ref, cb_ref, gw_ref, gb_ref, dr_ref, mg_ref, inw_hbm, outw_hbm, mi_hbm, mo_hbm, o_ref,
    xg, inw, outw, mi, wsrc, wt, acc, ss, ytab, ztab, mixed, op, oi, obox, res,
    xt, acc2, ss2, hid, po, abox, bbox, abox2, bbox2, give, got, send_sem, recv_sem, local_sem,
):
    tm, cw = x_ref.shape
    hm = tm // 2
    ch = gw_ref.shape[2]
    d = ng_ref.shape[1]
    rm = tm // 2
    ff = wsrc.shape[1] // NY
    lanes = d // (nz * NY)
    zl = NY * lanes
    nseq = nz * NY
    main = pl.ds(RIM, tm)

    s = lax.axis_index("seq")
    t = lax.axis_index("tensor")
    z, y = lax.div(s, NY), lax.rem(s, NY)
    x, c = lax.div(t, 2), lax.rem(t, 2)

    def dev(z_=None, y_=None, x_=None, c_=None):
        z_, y_ = (z if z_ is None else z_), (y if y_ is None else y_)
        x_, c_ = (x if x_ is None else x_), (c if c_ is None else c_)
        return (z_ * NY + y_, x_ * 2 + c_)

    along_x = lambda i: dev(x_=i)
    along_y = lambda j: dev(y_=j)
    sibling = dev(c_=1 - c)
    xn, xp, xo = mod(x + 1, NX), mod(x + 3, NX), mod(x + 2, NX)
    yn, yp, yo = mod(y + 1, NY), mod(y + 3, NY), mod(y + 2, NY)
    after, before = mod(s + 1, nseq), mod(s + nseq - 1, nseq)

    loads = {}
    for number, (name, src, dst) in enumerate(
        (("inw", inw_hbm, inw), ("outw", outw_hbm, outw), ("mi", mi_hbm, mi), ("mo", mo_hbm, wsrc.at[2]))
    ):
        loads[name] = pltpu.make_async_copy(src, dst, local_sem.at[number])
    for name in ("mi", "mo", "inw", "outw"):
        loads[name].start()

    barrier = pltpu.get_barrier_semaphore()
    partners = [dev(x_=xn), dev(x_=xp), sibling]
    partners += [(near, mod(t + n, 8)) for near in (after, before) for n in range(8)]
    partners += [dev(y_=mod(y + k, NY)) for k in range(1, NY)]
    partners += [dev(z_=mod(z + k, nz)) for k in range(1, nz)]
    for partner in partners:
        pl.semaphore_signal(barrier, inc=1, device_id=partner, device_id_type=pl.DeviceIdType.MESH)
    pl.semaphore_wait(barrier, len(partners))

    wire = Wire(send_sem, recv_sem)

    def x_piece(i, h):
        return xg.at[i * 2 + c, pl.ds(RIM + h * hm, hm)]

    lot = wire.lot(xg.at[0, pl.ds(0, 8 * RIM)])
    rims = []
    for n in range(8):
        rims.append(
            lot.message(
                x_ref.at[pl.ds(tm - RIM, RIM)], xg.at[t, pl.ds(0, RIM)], xg.at[mod(t + 8 - n, 8), pl.ds(0, RIM)],
                (after, mod(t + n, 8)),
            )
        )
        rims[-1].start()

    def rim_of(b):
        n = mod(t + 8 - b, 8)
        pltpu.make_async_remote_copy(
            src_ref=x_ref.at[pl.ds(tm - RIM, RIM)],
            dst_ref=xg.at[b, pl.ds(0, RIM)],
            send_sem=send_sem.at[0],
            recv_sem=recv_sem.at[n],
            device_id=(after, t),
            device_id_type=pl.DeviceIdType.MESH,
        ).wait_recv()

    xring = Spread(wire.lot(obox), x_piece, x, along_x, own=lambda h: x_ref.at[pl.ds(h * hm, hm)])
    xring.start()
    to_sib = {}
    lot = wire.lot(oi)
    for name, i in (("own", x), ("prv", xp), ("nxt", xn), ("opp", xo)):
        src = x_ref if name == "own" else xg.at[i * 2 + c, main]
        to_sib[name] = lot.message(src, xg.at[i * 2 + c, main], xg.at[i * 2 + 1 - c, main], sibling)
    to_sib["own"].start()
    xg[t, main] = x_ref[...]

    loads["mi"].wait()
    for g in range(2):
        wsrc[g] = mi[g].astype(F32).T.astype(BF16)
    loads["mo"].wait()

    zn, zp = mod(z + 1, nz), mod(z + nz - 1, nz)
    steps = nz // 2
    assert steps > 1

    class Weights:
        def __init__(self, first, count):
            self.group = pl.ds(first, count)
            self.over_y, self.up, self.down = [], [[]], [[]]
            self.ring = wire.lot(self.lanes(0, 0, (3 * NY - 1) * lanes + (nz - 1) * zl - 2 * zl))
            self.pair = wire.lot(self.lanes(0, 0, d))
            for k in range(1, NY):
                j, src_y = mod(y + k, NY), mod(y + NY - k, NY)
                self.over_y.append(
                    self.ring.message(
                        self.rows(j), self.lanes(0, s * lanes, lanes), self.lanes(0, (z * NY + src_y) * lanes, lanes),
                        along_y(j),
                    )
                )
            rise, fall = wire.arrival(), wire.arrival()
            self.hop_1 = (rise, fall)
            self.sib_all = wire.arrival()
            for k in range(NY):
                at = mod(y + NY - k, NY) * lanes
                here = self.lanes(0, z * zl + at, lanes)
                src = self.rows(y) if k == 0 else here
                self.up[0].append(self.ring.message(src, here, None, dev(z_=zn), rise))
                self.down[0].append(self.ring.message(src, here, None, dev(z_=zp), fall))
            self.to_sib = [[self.sib(z * zl, zl)]]
            for k in range(1, steps + 1):
                half = zl // 2 if k == steps else zl
                up, up_in = mod(z + nz - (k - 1), nz) * zl, mod(z + nz - k, nz) * zl
                down, down_in = mod(z + k - 1, nz) * zl + zl - half, mod(z + k, nz) * zl + zl - half
                if k > 1:
                    here, there = self.lanes(0, up, half), self.lanes(0, up_in, half)
                    self.up.append([self.ring.message(here, here, there, dev(z_=zn))])
                    here, there = self.lanes(0, down, half), self.lanes(0, down_in, half)
                    self.down.append([self.ring.message(here, here, there, dev(z_=zp))])
                self.to_sib.append([self.sib(up_in, half), self.sib(down_in, half)])

        def rows(self, j):
            return wsrc.at[self.group, pl.ds(pl.multiple_of(j * ff, 16), ff)]

        def lanes(self, slot, start, size):
            return wt.at[self.group, pl.ds(slot * ff, ff), pl.ds(pl.multiple_of(start, 128), size)]

        def sib(self, start, size):
            return self.pair.message(
                self.lanes(0, start, size), self.lanes(1, start, size), None, sibling, self.sib_all
            )

        def split(self):
            for k in (0, 2, 1):
                self.over_y[k].start()

        def first(self, k):
            if k > 0:
                self.over_y[k - 1].arrived()
            self.up[0][k].start()
            self.down[0][k].start()

        def own_to_sib(self):
            self.to_sib[0][0].start()

        def step(self, k):
            for ring, n in ((self.up, 0), (self.down, 1)):
                if k == 1:
                    arrived(self.hop_1[n], self.lanes(0, 0, zl))
                else:
                    ring[k - 1][0].arrived()
                if k < steps:
                    ring[k][0].start()
            for message in self.to_sib[k]:
                message.start()

        def finish(self):
            arrived(self.sib_all, self.lanes(1, 0, d))

    w_in, w_down = Weights(0, 2), Weights(2, 1)
    w_in.split()
    w_in.first(0)
    w_down.split()
    wt[:, pl.ds(0, ff), pl.ds(pl.multiple_of(s * lanes, 128), lanes)] = wsrc[:, pl.ds(pl.multiple_of(y * ff, 16), ff)]

    acc[...] = jnp.zeros_like(acc)
    ss[...] = jnp.zeros_like(ss)
    loads["inw"].wait()
    order = [t, x * 2 + 1 - c, xp * 2 + c, xn * 2 + c, xp * 2 + 1 - c, xn * 2 + 1 - c, xo * 2 + c, xo * 2 + 1 - c]

    def step_2():
        xring.forward()
        xring.prv_done()
        to_sib["prv"].start()
        w_in.first(1)
        w_in.first(3)

    def step_3():
        xring.nxt_done()
        to_sib["nxt"].start()
        w_in.first(2)

    def step_6():
        xring.opp_done()
        to_sib["opp"].start()
        for k in range(NY):
            w_down.first(k)

    arrivals = {
        1: to_sib["own"].arrived,
        2: step_2,
        3: step_3,
        4: to_sib["prv"].arrived,
        5: to_sib["nxt"].arrived,
        6: step_6,
        7: to_sib["opp"].arrived,
    }

    def take(k, _):
        at_step(k, arrivals)
        b = picked(k, order)
        rim_of(b)
        at = pl.multiple_of(b * cw, 128)
        block = xg[b].astype(F32)
        ss[...] += lane_sums(block * block)
        scaled = (block * ng_ref[:, pl.ds(at, cw)]).astype(BF16)
        for g in range(2):
            acc[g] += jnp.dot(scaled, inw[g, pl.ds(at, cw)], preferred_element_type=F32)
        return 0

    lax.fori_loop(0, 8, take, 0)
    scale = lax.rsqrt(jnp.sum(ss[...], axis=1, keepdims=True) * (1.0 / d) + EPS)
    w_in.own_to_sib()
    w_down.own_to_sib()
    branch_x = (acc[0] * scale).astype(BF16).astype(F32)
    known = jnp.logical_or(s > 0, lax.broadcasted_iota(jnp.int32, branch_x.shape, 0) >= RIM)
    branch_x = jnp.where(known, branch_x, 0.0)
    acc[1] = jax.nn.gelu(acc[1] * scale, approximate=True)

    convolved = jnp.zeros((tm, ch), F32) + cb_ref[...]
    for k in range(cw_ref.shape[0]):
        convolved = convolved + cw_ref[k : k + 1] * pltpu.roll(branch_x, k, 0)[RIM:]
    conv_out = convolved.astype(BF16)
    gates = [
        jnp.dot(conv_out, gw_ref[g, 0], preferred_element_type=F32) + gb_ref[g : g + 1] for g in range(2)
    ]
    log_decay = -8.0 * jax.nn.sigmoid(gates[0]) * dr_ref[...]
    decay = jnp.exp(log_decay)
    driven = conv_out.astype(F32) * jax.nn.sigmoid(gates[1]) * jnp.sqrt(expm1_negated(2.0 * log_decay))
    row = lax.broadcasted_iota(jnp.int32, (tm, ch), 0)
    step = 1
    while step < tm:
        inside = row >= step
        driven = driven + decay * jnp.where(inside, pltpu.roll(driven, step, 0), 0.0)
        decay = decay * jnp.where(inside, pltpu.roll(decay, step, 0), 1.0)
        step *= 2
    ytab[y, 0:1] = decay[tm - 1 :]
    ytab[y, 1:2] = driven[tm - 1 :]
    over_y = []
    lot, there = wire.lot(ytab.at[pl.ds(0, NY - 1)]), wire.arrival()
    for k in range(1, NY):
        over_y.append(
            lot.message(ytab.at[y], ytab.at[y], None, along_y(mod(y + k, NY)), there)
        )
        over_y[-1].start()
    arrived(there, ytab.at[pl.ds(0, NY - 1)])
    total_a, total_b = jnp.ones((1, ch), F32), jnp.zeros((1, ch), F32)
    before_a, before_b = total_a, total_b
    for j in range(NY):
        a, b = ytab[j, 0:1], ytab[j, 1:2]
        before_b = jnp.where(j < y, a * before_b + b, before_b)
        before_a = jnp.where(j < y, a * before_a, before_a)
        total_b = a * total_b + b
        total_a = a * total_a
    ztab[z, 0:1] = total_a
    ztab[z, 1:2] = total_b
    over_z = []
    lot, there = wire.lot(ztab.at[pl.ds(0, nz - 1)]), wire.arrival()
    for k in range(1, nz):
        over_z.append(
            lot.message(ztab.at[z], ztab.at[z], None, dev(z_=mod(z + k, nz)), there)
        )
        over_z[-1].start()
    arrived(there, ztab.at[pl.ds(0, nz - 1)])
    carry = jnp.zeros((1, ch), F32)
    for j in range(nz):
        carry = jnp.where(j < z, ztab[j, 0:1] * carry + ztab[j, 1:2], carry)
    carry = before_a * carry + before_b
    mixed[...] = ((decay * carry + driven) * acc[1, RIM:]).astype(BF16)
    w_in.step(1)
    w_down.step(1)

    loads["outw"].wait()
    columns = (xo, xn, xp, x)

    def block(i):
        return pl.ds(pl.multiple_of(i * cw, 128), cw)

    over_d2d = []
    lot = wire.lot(oi)
    for n, i in enumerate(columns):
        for core in (1 - c, c):
            at = pl.multiple_of((i * 2 + core) * cw, 128)
            part = jnp.dot(mixed[...], outw[:, pl.ds(at, cw)], preferred_element_type=F32)
            op[core, :, block(i)] = part.astype(BF16)
            if core is not c:
                over_d2d.append(lot.message(op.at[1 - c, :, block(i)], oi.at[n], oi.at[n], sibling))
                over_d2d[-1].start()

    out_ring = Gathered(wire.lot(obox), lambda i, h: op.at[c, pl.ds(h * hm, hm), block(i)], x, along_x, obox)
    starts = (out_ring.start_far, out_ring.start_next, out_ring.start_prev, lambda: None)
    for n, i in enumerate(columns):
        over_d2d[n].arrived()
        op[c, :, block(i)] = (op[c, :, block(i)].astype(F32) + oi[n].astype(F32)).astype(BF16)
        starts[n]()
    out_ring.relay()
    if steps > 2:
        w_in.step(2)
    for h, value in enumerate(out_ring.result()):
        rows = pl.ds(h * hm, hm)
        res[rows] = (x_ref[rows].astype(F32) + value).astype(BF16)

    hg = rm // GROUPS
    hh = hg // 2
    other = 1 - c

    def token(j, h=None):
        if h is None:
            return pl.ds(pl.multiple_of(j * hg, 16), hg)
        return pl.ds(pl.multiple_of(j * hg + h * hh, 16), hh)

    def of_core(core, g, size, h=0):
        return pl.ds(pl.multiple_of(core * rm + g * hg + h * hh, 16), size)

    here_rows = pl.ds(pl.multiple_of(y * hg, 16), hg)

    class Rows:
        def __init__(self, g):
            self.g = g
            there = xt.at[1 - c, g, here_rows, block(x)]
            lot = wire.lot(xt.at[0, :, pl.ds(0, 30 * hg // (NX * GROUPS))])
            self.swap = wire.lot(there).message(res.at[of_core(other, g, hg)], xt.at[c, g, here_rows, block(x)], there, sibling)
            size = lambda n: xt.at[0, 0, pl.ds(0, n * hg), pl.ds(0, cw)]
            self.b_far, self.size = wire.arrival(), size

            def ring(core, rows, wholes, columns_of, me, device_of, far=None):
                return Around(
                    lot,
                    lambda m, h: xt.at[core, g, rows(m, h), columns_of(m)],
                    lambda m: xt.at[core, g, wholes(m), columns_of(m)],
                    size, me, device_of, far,
                )

            def over_x(core, j, far=None):
                return ring(core, lambda m, h: token(j, h), lambda m: token(j), block, x, along_x, far)

            def over_y(core, i):
                return ring(core, token, token, lambda m: block(i), y, along_y)

            self.a_x, self.b_y = over_x(c, y), over_y(other, x)
            self.a_y = [over_y(c, i) for i in (x, xp, xn, xo)]
            self.b_x = [over_x(other, j, self.b_far) for j in (y, yp, yn, yo)]

        def begin(self):
            self.swap.start()
            xt[c, self.g, here_rows, block(x)] = res[of_core(c, self.g, hg)]
            self.a_x.start()

        def begin_other(self):
            self.swap.arrived()
            self.b_y.start()

        def own(self):
            self.a_y[0].start()
            self.b_x[0].start()

        def relay_first(self):
            self.a_x.forward()
            self.b_y.forward()

        def sides(self):
            for n in (1, 2):
                self.a_y[n].start()
                self.b_x[n].start()

        def far(self):
            self.a_x.opp_done()
            self.a_y[3].start()
            self.b_y.opp_done()
            self.b_x[3].start()

        def relay(self, n):
            self.a_y[n].forward()
            self.b_x[n].forward()

        def a_done(self, n):
            self.a_y[n].opp_done()

        def b_done(self):
            arrived(self.b_far, self.size(4))

    class Sums:
        def __init__(self, g):
            self.g = g
            lot = wire.lot(po.at[0, :, pl.ds(0, 60 * hh // (NX * GROUPS))])
            self.a = [
                Gathered(lot, lambda j, h, i=i: po.at[c, g, token(j, h), block(i)], y, along_y, abox.at[g, n])
                for n, i in enumerate(columns)
            ]
            self.b = [
                Gathered(lot, lambda i, h, j=j: po.at[other, g, token(j, h), block(i)], x, along_x, bbox.at[g, n])
                for n, j in enumerate(b_rows)
            ]
            self.a_last = Gathered(lot, lambda i, h: po.at[c, g, token(y, h), block(i)], x, along_x, abox2.at[g])
            self.b_last = Gathered(lot, lambda j, h: po.at[other, g, token(j, h), block(x)], y, along_y, bbox2.at[g])
            self.back = wire.lot(give.at[g]).message(give.at[g], got.at[g], got.at[g], sibling)

        def a_all(self, n):
            self.a[n].start_far()
            self.a[n].start_next()
            self.a[n].start_prev()

        def b_all(self, method):
            for ring in self.b:
                getattr(ring, method)()

        def down(self):
            starts = (
                lambda: (self.a_all(0), self.b_all("start_far")),
                lambda: (self.a_all(1), self.b_all("start_next")),
                lambda: (self.a_all(2), self.b_all("start_prev")),
                lambda: self.a_all(3),
            )

            def one(k, _):
                i = picked(k, list(columns))
                both = pl.ds(pl.multiple_of(i * 2 * cw, 128), 2 * cw)
                part = jnp.dot(hid[...], wt[2, :, both], preferred_element_type=F32).astype(BF16)
                for core in range(2):
                    po[core, self.g, :, block(i)] = part[:, core * cw : (core + 1) * cw]
                at_step(k, dict(enumerate(starts)))
                return 0

            lax.fori_loop(0, 4, one, 0)

        def relay(self, n):
            self.a[n].relay()
            self.b[n].relay()

        def first_sums(self):
            a_starts = (self.a_last.start_far, self.a_last.start_next, self.a_last.start_prev, lambda: None)
            b_starts = (self.b_last.start_far, self.b_last.start_next, self.b_last.start_prev, lambda: None)
            for n in range(4):
                for ring, start, core, rows_at, i in (
                    (self.a[n], a_starts[n], c, y, columns[n]),
                    (self.b[n], b_starts[n], other, b_rows[n], x),
                ):
                    for h, value in enumerate(ring.result()):
                        po[core, self.g, token(rows_at, h), block(i)] = value.astype(BF16)
                    start()

        def relay_last(self):
            self.b_last.relay()
            self.a_last.relay()

        def results(self):
            for h, value in enumerate(self.b_last.result()):
                give[self.g, pl.ds(h * hh, hh)] = value.astype(BF16)
            self.back.start()
            for h, value in enumerate(self.a_last.result()):
                rows = of_core(c, self.g, hh, h)
                o_ref[rows] = (res[rows].astype(F32) + value).astype(BF16)

        def others(self):
            self.back.arrived()
            rows = of_core(other, self.g, hg)
            o_ref[rows] = (res[rows].astype(F32) + got[self.g].astype(F32)).astype(BF16)

    b_rows = (yo, yn, yp, y)
    rows_0, rows_1 = Rows(0), Rows(1)
    sums_0, sums_1 = Sums(0), Sums(1)

    def multiply(rows, extra):
        pairs = (((c, x), (other, x)), ((c, xp), (c, xn)), ((other, xp), (other, xn)), ((c, xo), (other, xo)))
        waits = {
            0: lambda: rows.a_done(0),
            1: lambda: (rows.a_done(1), rows.a_done(2)),
            3: lambda: (rows.a_done(3), rows.b_done()),
        }
        acc2[...] = jnp.zeros_like(acc2)
        ss2[...] = jnp.zeros_like(ss2)

        def one(k, _):
            at_step(k, extra)
            at_step(k, waits)
            scaled, weights, squares = [], [], 0.0
            for n in range(2):
                core, i = picked(k, [w[n][0] for w in pairs]), picked(k, [w[n][1] for w in pairs])
                at = pl.multiple_of((i * 2 + core) * cw, 128)
                block_rows = xt[core, rows.g, :, block(i)].astype(F32)
                squares = squares + lane_sums(block_rows * block_rows)
                scaled.append((block_rows * mg_ref[:, pl.ds(at, cw)]).astype(BF16))
                weights.append(wt[0:2, :, pl.ds(at, cw)].reshape(4 * ff, cw))
            ss2[...] += squares
            acc2[...] += lax.dot_general(
                jnp.concatenate(scaled, axis=1), jnp.concatenate(weights, axis=1), (((1,), (1,)), ((), ())),
                preferred_element_type=F32,
            )
            return 0

        lax.fori_loop(0, 4, one, 0)
        scale2 = lax.rsqrt(jnp.sum(ss2[...], axis=1, keepdims=True) * (1.0 / d) + EPS)
        hid[...] = (jax.nn.gelu(acc2[:, : 2 * ff] * scale2, approximate=True) * (acc2[:, 2 * ff :] * scale2)).astype(BF16)

    rows_0.begin()
    rows_0.begin_other()
    rows_0.own()
    rows_1.begin()
    rows_1.begin_other()
    rows_0.relay_first()
    rows_0.sides()
    rows_0.far()
    for k in range(3, steps):
        w_in.step(k)
    rows_0.relay(0)
    if steps > 2:
        w_down.step(2)
    rows_1.relay_first()
    rows_0.relay(1)
    rows_1.own()
    rows_0.relay(2)
    rows_1.sides()
    rows_0.relay(3)
    rows_1.far()
    w_in.step(steps)
    for k in range(3, steps):
        w_down.step(k)
    w_in.finish()
    multiply(rows_0, {n: functools.partial(rows_1.relay, n) for n in range(4)})
    w_down.step(steps)
    w_down.finish()
    sums_0.down()
    multiply(rows_1, {n: functools.partial(sums_0.relay, n) for n in range(4)})
    sums_1.down()
    sums_0.first_sums()
    for n in range(4):
        sums_1.relay(n)
    sums_0.relay_last()
    sums_1.first_sums()
    sums_0.results()
    sums_1.relay_last()
    sums_0.others()
    sums_1.results()
    sums_1.others()
    wire.drain()


def shards(
    nz, layer_input, norm_gain, in_weights, conv_weight, conv_bias, gate_weights, gate_bias, decay_rate, out_weight,
    mlp_gain, mlp_in, mlp_out,
):
    tm, cw = layer_input.shape
    d, ch = in_weights.shape[1:]
    units = mlp_out.shape[0]
    ff = units // NY
    hg = tm // 2 // GROUPS
    vmem = pl.BlockSpec(memory_space=pltpu.VMEM)
    hbm = pl.BlockSpec(memory_space=pl.ANY)
    scratch = [
        ((8, RIM + tm, cw), BF16),
        ((2, d, ch), BF16),
        ((ch, d), BF16),
        (mlp_in.shape, BF16),
        ((3, units, mlp_in.shape[1]), BF16),
        ((3, 2 * ff, d), BF16),
        ((2, RIM + tm, ch), F32),
        ((RIM + tm, 128), F32),
        ((NY, 2, ch), F32),
        ((nz, 2, ch), F32),
        ((tm, ch), BF16),
        ((2, tm, NX * cw), BF16),
        ((4, tm, cw), BF16),
        ((6, tm // 2, cw), BF16),
        ((tm, cw), BF16),
        ((2, GROUPS, NY * hg, NX * cw), BF16),
        ((NY * hg, 4 * ff), F32),
        ((NY * hg, 128), F32),
        ((NY * hg, 2 * ff), BF16),
        ((2, GROUPS, NY * hg, NX * cw), BF16),
        ((GROUPS, 4, 6, hg // 2, cw), BF16),
        ((GROUPS, 4, 6, hg // 2, cw), BF16),
        ((GROUPS, 6, hg // 2, cw), BF16),
        ((GROUPS, 6, hg // 2, cw), BF16),
        ((GROUPS, hg, cw), BF16),
        ((GROUPS, hg, cw), BF16),
    ]
    call = pl.pallas_call(
        functools.partial(kernel, nz),
        out_shape=jax.ShapeDtypeStruct((tm, cw), BF16),
        in_specs=[vmem] * 8 + [hbm] * 4,
        out_specs=vmem,
        scratch_shapes=[pltpu.VMEM(shape, dtype) for shape, dtype in scratch]
        + [
            pltpu.SemaphoreType.DMA((32,)),
            pltpu.SemaphoreType.DMA((ARRIVALS,)),
            pltpu.SemaphoreType.DMA((4,)),
        ],
        compiler_params=pltpu.CompilerParams(
            collective_id=0, has_side_effects=True, vmem_limit_bytes=56 * 1024 * 1024
        ),
    )
    return call(
        layer_input, norm_gain[None], conv_weight, conv_bias[None], gate_weights, gate_bias, decay_rate[None],
        mlp_gain[None], in_weights, out_weight, mlp_in, mlp_out,
    )


def solution(mesh):
    return jax.shard_map(
        functools.partial(shards, mesh.shape["seq"] // NY),
        mesh=mesh,
        in_specs=(
            P("seq", "tensor"),
            P(),
            P(None, None, "tensor"),
            P(None, "tensor"),
            P("tensor"),
            P(None, "tensor", None, None),
            P(None, "tensor"),
            P("tensor"),
            P("tensor", None),
            P(),
            P(None, "seq", "tensor"),
            P("tensor", "seq"),
        ),
        out_specs=P("seq", "tensor"),
        check_vma=False,
    )
```

```python
import functools

import jax
import jax.numpy as jnp
from jax import lax
from jax.experimental import pallas as pl
from jax.experimental.pallas import tpu as pltpu
from jax.sharding import PartitionSpec as P

NY = 4
NX = 4
EPS = 1e-06
F32 = jnp.float32
BF16 = jnp.bfloat16
ARRIVALS = 128
LOTS = 19
RIM = 8
GROUPS = 2


def mod(value, size):
    return lax.rem(value + size, size)


def expm1_negated(v):
    series = 1.0 + v * (1.0 / 9.0)
    for n in range(8, 1, -1):
        series = 1.0 + v * (1.0 / n) * series
    return jnp.where(v > -0.5, -v * series, 1.0 - jnp.exp(v))


class Wire:
    def __init__(self, send, recv):
        self.send, self.recv, self.used, self.lots = send, recv, 0, []

    def arrival(self):
        self.used += 1
        return self.recv.at[self.used - 1]

    def lot(self, whole):
        self.lots.append(whole)
        return Lot(self, len(self.lots) - 1)

    def drain(self):
        for number, whole in enumerate(self.lots):
            pltpu.make_async_copy(whole, whole, self.send.at[number]).wait()


class Lot:
    def __init__(self, wire, number):
        self.wire, self.number = wire, number

    def message(self, src, dst, landing, device, arrival=None):
        arrival = self.wire.arrival() if arrival is None else arrival
        return Message(self.wire.send.at[self.number], arrival, src, dst, landing, device)


def arrived(semaphore, whole):
    pltpu.make_async_copy(whole, whole, semaphore).wait()


class Message:
    def __init__(self, send, recv, src, dst, landing, device):
        self.send, self.recv, self.src, self.dst, self.landing, self.device = send, recv, src, dst, landing, device

    def copy(self, dst):
        return pltpu.make_async_remote_copy(
            src_ref=self.src,
            dst_ref=dst,
            send_sem=self.send,
            recv_sem=self.recv,
            device_id=self.device,
            device_id_type=pl.DeviceIdType.MESH,
        )

    def start(self):
        self.copy(self.dst).start()

    def arrived(self):
        self.copy(self.landing).wait_recv()


class Spread:
    def __init__(self, lot, piece, me, device_of, own=None):
        nxt, prv, opp = mod(me + 1, 4), mod(me + 3, 4), mod(me + 2, 4)
        own = own or (lambda h: piece(me, h))
        self.na = lot.message(own(0), piece(me, 0), piece(prv, 0), device_of(nxt))
        self.nb = lot.message(own(1), piece(me, 1), piece(prv, 1), device_of(nxt))
        self.pb = lot.message(own(1), piece(me, 1), piece(nxt, 1), device_of(prv))
        self.pa = lot.message(own(0), piece(me, 0), piece(nxt, 0), device_of(prv))
        self.fn = lot.message(piece(prv, 0), piece(prv, 0), piece(opp, 0), device_of(nxt))
        self.fp = lot.message(piece(nxt, 1), piece(nxt, 1), piece(opp, 1), device_of(prv))

    def start(self):
        self.na.start()
        self.pb.start()
        self.nb.start()
        self.pa.start()

    def forward(self):
        self.na.arrived()
        self.fn.start()
        self.pb.arrived()
        self.fp.start()

    def prv_done(self):
        self.nb.arrived()

    def nxt_done(self):
        self.pa.arrived()

    def opp_done(self):
        self.fn.arrived()
        self.fp.arrived()


class Around:
    def __init__(self, lot, piece, part, size, me, device_of, far=None):
        nxt, prv, opp = mod(me + 1, 4), mod(me + 3, 4), mod(me + 2, 4)
        self.near, self.size = lot.wire.arrival(), size
        self.far = lot.wire.arrival() if far is None else far
        self.n = lot.message(part(me), part(me), None, device_of(nxt), self.near)
        self.p = lot.message(part(me), part(me), None, device_of(prv), self.near)
        self.fn = lot.message(piece(prv, 0), piece(prv, 0), None, device_of(nxt), self.far)
        self.fp = lot.message(piece(nxt, 1), piece(nxt, 1), None, device_of(prv), self.far)

    def start(self):
        self.n.start()
        self.p.start()

    def forward(self):
        arrived(self.near, self.size(2))
        self.fn.start()
        self.fp.start()

    def opp_done(self):
        arrived(self.far, self.size(1))


class Gathered:
    def __init__(self, lot, part, me, device_of, box):
        nxt, prv, opp = mod(me + 1, 4), mod(me + 3, 4), mod(me + 2, 4)
        self.part, self.me, self.nxt, self.prv, self.box = part, me, nxt, prv, box
        self.first, self.last = lot.wire.arrival(), lot.wire.arrival()

        def send(src, slot, device):
            return lot.message(src, box.at[slot], None, device, self.first if slot < 2 else self.last)

        self.oa = send(part(opp, 0), 0, device_of(nxt))
        self.ob = send(part(opp, 1), 1, device_of(prv))
        self.db = send(part(nxt, 1), 2, device_of(nxt))
        self.da = send(part(prv, 0), 3, device_of(prv))
        self.ca = send(part(nxt, 0), 4, device_of(nxt))
        self.cb = send(part(prv, 1), 5, device_of(prv))

    def start_far(self):
        self.oa.start()
        self.ob.start()

    def start_next(self):
        self.db.start()

    def start_prev(self):
        self.da.start()

    def relay(self):
        arrived(self.first, self.box.at[pl.ds(0, 2)])
        for leaving, member, half, slot in ((self.ca, self.nxt, 0, 0), (self.cb, self.prv, 1, 1)):
            ref = self.part(member, half)
            ref[...] = (ref[...].astype(F32) + self.box[slot].astype(F32)).astype(BF16)
            leaving.start()

    def result(self):
        arrived(self.last, self.box.at[pl.ds(2, 4)])
        halves = []
        for half, slots in ((0, (4, 3)), (1, (2, 5))):
            value = self.part(self.me, half)[...].astype(F32)
            for slot in slots:
                value = value + self.box[slot].astype(F32)
            halves.append(value)
        return halves


def lane_sums(value):
    return sum(value[:, at : at + 128] for at in range(128, value.shape[1], 128)) + value[:, :128]


def at_step(k, steps):
    for number, step in steps.items():

        def run(step=step):
            step()

        pl.when(k == number)(run)


def picked(k, values):
    result = values[0]
    for n in range(1, len(values)):
        result = jnp.where(k == n, values[n], result)
    return result


def kernel(
    nz, x_ref, ng_ref, cw_ref, cb_ref, gw_ref, gb_ref, dr_ref, mg_ref, inw_hbm, outw_hbm, mi_hbm, mo_hbm, o_ref,
    xg, inw, outw, mi, wsrc, wt, acc, ss, ytab, ztab, mixed, op, oi, obox, res,
    xt, acc2, ss2, hid, po, abox, bbox, abox2, bbox2, give, got, send_sem, recv_sem, local_sem,
):
    tm, cw = x_ref.shape
    hm = tm // 2
    ch = gw_ref.shape[2]
    d = ng_ref.shape[1]
    rm = tm // 2
    ff = wsrc.shape[1] // NY
    lanes = d // (nz * NY)
    zl = NY * lanes
    nseq = nz * NY
    main = pl.ds(RIM, tm)

    s = lax.axis_index("seq")
    t = lax.axis_index("tensor")
    z, y = lax.div(s, NY), lax.rem(s, NY)
    x, c = lax.div(t, 2), lax.rem(t, 2)

    def dev(z_=None, y_=None, x_=None, c_=None):
        z_, y_ = (z if z_ is None else z_), (y if y_ is None else y_)
        x_, c_ = (x if x_ is None else x_), (c if c_ is None else c_)
        return (z_ * NY + y_, x_ * 2 + c_)

    along_x = lambda i: dev(x_=i)
    along_y = lambda j: dev(y_=j)
    sibling = dev(c_=1 - c)
    xn, xp, xo = mod(x + 1, NX), mod(x + 3, NX), mod(x + 2, NX)
    yn, yp, yo = mod(y + 1, NY), mod(y + 3, NY), mod(y + 2, NY)
    after, before = mod(s + 1, nseq), mod(s + nseq - 1, nseq)

    loads = {}
    for number, (name, src, dst) in enumerate(
        (("inw", inw_hbm, inw), ("outw", outw_hbm, outw), ("mi", mi_hbm, mi), ("mo", mo_hbm, wsrc.at[2]))
    ):
        loads[name] = pltpu.make_async_copy(src, dst, local_sem.at[number])
    for name in ("mi", "mo", "inw", "outw"):
        loads[name].start()

    barrier = pltpu.get_barrier_semaphore()
    partners = [dev(x_=xn), dev(x_=xp), sibling]
    partners += [(near, mod(t + n, 8)) for near in (after, before) for n in range(8)]
    partners += [dev(y_=mod(y + k, NY)) for k in range(1, NY)]
    partners += [dev(z_=mod(z + k, nz)) for k in range(1, nz)]
    for partner in partners:
        pl.semaphore_signal(barrier, inc=1, device_id=partner, device_id_type=pl.DeviceIdType.MESH)
    loads["mi"].wait()
    for g in range(2):
        wsrc[g] = mi[g].astype(F32).T.astype(BF16)
    loads["mo"].wait()
    pl.semaphore_wait(barrier, len(partners))

    wire = Wire(send_sem, recv_sem)

    def x_piece(i, h):
        return xg.at[i * 2 + c, pl.ds(RIM + h * hm, hm)]

    lot = wire.lot(xg.at[0, pl.ds(0, 8 * RIM)])
    rims = []
    for n in range(8):
        rims.append(
            lot.message(
                x_ref.at[pl.ds(tm - RIM, RIM)], xg.at[t, pl.ds(0, RIM)], xg.at[mod(t + 8 - n, 8), pl.ds(0, RIM)],
                (after, mod(t + n, 8)),
            )
        )
        rims[-1].start()

    def rim_of(b):
        n = mod(t + 8 - b, 8)
        pltpu.make_async_remote_copy(
            src_ref=x_ref.at[pl.ds(tm - RIM, RIM)],
            dst_ref=xg.at[b, pl.ds(0, RIM)],
            send_sem=send_sem.at[0],
            recv_sem=recv_sem.at[n],
            device_id=(after, t),
            device_id_type=pl.DeviceIdType.MESH,
        ).wait_recv()

    xring = Spread(wire.lot(obox), x_piece, x, along_x, own=lambda h: x_ref.at[pl.ds(h * hm, hm)])
    xring.start()
    to_sib = {}
    lot = wire.lot(oi)
    for name, i in (("own", x), ("prv", xp), ("nxt", xn), ("opp", xo)):
        src = x_ref if name == "own" else xg.at[i * 2 + c, main]
        to_sib[name] = lot.message(src, xg.at[i * 2 + c, main], xg.at[i * 2 + 1 - c, main], sibling)
    to_sib["own"].start()
    xg[t, main] = x_ref[...]

    zn, zp = mod(z + 1, nz), mod(z + nz - 1, nz)
    steps = nz // 2
    assert steps > 1

    class Weights:
        def __init__(self, first, count):
            self.group = pl.ds(first, count)
            self.over_y, self.up, self.down = [], [[]], [[]]
            self.ring = wire.lot(self.lanes(0, 0, (3 * NY - 1) * lanes + (nz - 1) * zl - 2 * zl))
            self.pair = wire.lot(self.lanes(0, 0, d))
            for k in range(1, NY):
                j, src_y = mod(y + k, NY), mod(y + NY - k, NY)
                self.over_y.append(
                    self.ring.message(
                        self.rows(j), self.lanes(0, s * lanes, lanes), self.lanes(0, (z * NY + src_y) * lanes, lanes),
                        along_y(j),
                    )
                )
            rise, fall = wire.arrival(), wire.arrival()
            self.hop_1 = (rise, fall)
            self.sib_all = wire.arrival()
            for k in range(NY):
                at = mod(y + NY - k, NY) * lanes
                here = self.lanes(0, z * zl + at, lanes)
                src = self.rows(y) if k == 0 else here
                self.up[0].append(self.ring.message(src, here, None, dev(z_=zn), rise))
                self.down[0].append(self.ring.message(src, here, None, dev(z_=zp), fall))
            self.to_sib = [[self.sib(z * zl, zl)]]
            for k in range(1, steps + 1):
                half = zl // 2 if k == steps else zl
                up, up_in = mod(z + nz - (k - 1), nz) * zl, mod(z + nz - k, nz) * zl
                down, down_in = mod(z + k - 1, nz) * zl + zl - half, mod(z + k, nz) * zl + zl - half
                if k > 1:
                    here, there = self.lanes(0, up, half), self.lanes(0, up_in, half)
                    self.up.append([self.ring.message(here, here, there, dev(z_=zn))])
                    here, there = self.lanes(0, down, half), self.lanes(0, down_in, half)
                    self.down.append([self.ring.message(here, here, there, dev(z_=zp))])
                self.to_sib.append([self.sib(up_in, half), self.sib(down_in, half)])

        def rows(self, j):
            return wsrc.at[self.group, pl.ds(pl.multiple_of(j * ff, 16), ff)]

        def lanes(self, slot, start, size):
            return wt.at[self.group, pl.ds(slot * ff, ff), pl.ds(pl.multiple_of(start, 128), size)]

        def sib(self, start, size):
            return self.pair.message(
                self.lanes(0, start, size), self.lanes(1, start, size), None, sibling, self.sib_all
            )

        def split(self):
            for k in (0, 2, 1):
                self.over_y[k].start()

        def first(self, k):
            if k > 0:
                self.over_y[k - 1].arrived()
            self.up[0][k].start()
            self.down[0][k].start()

        def own_to_sib(self):
            self.to_sib[0][0].start()

        def step(self, k):
            for ring, n in ((self.up, 0), (self.down, 1)):
                if k == 1:
                    arrived(self.hop_1[n], self.lanes(0, 0, zl))
                else:
                    ring[k - 1][0].arrived()
                if k < steps:
                    ring[k][0].start()
            for message in self.to_sib[k]:
                message.start()

        def finish(self):
            arrived(self.sib_all, self.lanes(1, 0, d))

    w_in, w_down = Weights(0, 2), Weights(2, 1)
    w_in.split()
    w_in.first(0)
    w_down.split()
    wt[:, pl.ds(0, ff), pl.ds(pl.multiple_of(s * lanes, 128), lanes)] = wsrc[:, pl.ds(pl.multiple_of(y * ff, 16), ff)]

    acc[...] = jnp.zeros_like(acc)
    ss[...] = jnp.zeros_like(ss)
    loads["inw"].wait()
    order = [t, x * 2 + 1 - c, xp * 2 + c, xn * 2 + c, xp * 2 + 1 - c, xn * 2 + 1 - c, xo * 2 + c, xo * 2 + 1 - c]

    def step_2():
        xring.forward()
        xring.prv_done()
        to_sib["prv"].start()
        w_in.first(1)
        w_in.first(3)

    def step_3():
        xring.nxt_done()
        to_sib["nxt"].start()
        w_in.first(2)

    def step_6():
        xring.opp_done()
        to_sib["opp"].start()
        for k in range(NY):
            w_down.first(k)

    arrivals = {
        1: to_sib["own"].arrived,
        2: step_2,
        3: step_3,
        4: to_sib["prv"].arrived,
        5: to_sib["nxt"].arrived,
        6: step_6,
        7: to_sib["opp"].arrived,
    }

    def take(k, _):
        at_step(k, arrivals)
        b = picked(k, order)
        rim_of(b)
        at = pl.multiple_of(b * cw, 128)
        block = xg[b].astype(F32)
        ss[...] += lane_sums(block * block)
        scaled = (block * ng_ref[:, pl.ds(at, cw)]).astype(BF16)
        for g in range(2):
            acc[g] += jnp.dot(scaled, inw[g, pl.ds(at, cw)], preferred_element_type=F32)
        return 0

    lax.fori_loop(0, 8, take, 0)
    scale = lax.rsqrt(jnp.sum(ss[...], axis=1, keepdims=True) * (1.0 / d) + EPS)
    w_in.own_to_sib()
    w_down.own_to_sib()
    branch_x = (acc[0] * scale).astype(BF16).astype(F32)
    known = jnp.logical_or(s > 0, lax.broadcasted_iota(jnp.int32, branch_x.shape, 0) >= RIM)
    branch_x = jnp.where(known, branch_x, 0.0)
    acc[1] = jax.nn.gelu(acc[1] * scale, approximate=True)

    convolved = jnp.zeros((tm, ch), F32) + cb_ref[...]
    for k in range(cw_ref.shape[0]):
        convolved = convolved + cw_ref[k : k + 1] * pltpu.roll(branch_x, k, 0)[RIM:]
    conv_out = convolved.astype(BF16)
    gates = [
        jnp.dot(conv_out, gw_ref[g, 0], preferred_element_type=F32) + gb_ref[g : g + 1] for g in range(2)
    ]
    log_decay = -8.0 * jax.nn.sigmoid(gates[0]) * dr_ref[...]
    decay = jnp.exp(log_decay)
    driven = conv_out.astype(F32) * jax.nn.sigmoid(gates[1]) * jnp.sqrt(expm1_negated(2.0 * log_decay))
    row = lax.broadcasted_iota(jnp.int32, (tm, ch), 0)
    step = 1
    while step < tm:
        inside = row >= step
        driven = driven + decay * jnp.where(inside, pltpu.roll(driven, step, 0), 0.0)
        decay = decay * jnp.where(inside, pltpu.roll(decay, step, 0), 1.0)
        step *= 2
    ytab[y, 0:1] = decay[tm - 1 :]
    ytab[y, 1:2] = driven[tm - 1 :]
    over_y = []
    lot, there = wire.lot(ytab.at[pl.ds(0, NY - 1)]), wire.arrival()
    for k in range(1, NY):
        over_y.append(
            lot.message(ytab.at[y], ytab.at[y], None, along_y(mod(y + k, NY)), there)
        )
        over_y[-1].start()
    arrived(there, ytab.at[pl.ds(0, NY - 1)])
    total_a, total_b = jnp.ones((1, ch), F32), jnp.zeros((1, ch), F32)
    before_a, before_b = total_a, total_b
    for j in range(NY):
        a, b = ytab[j, 0:1], ytab[j, 1:2]
        before_b = jnp.where(j < y, a * before_b + b, before_b)
        before_a = jnp.where(j < y, a * before_a, before_a)
        total_b = a * total_b + b
        total_a = a * total_a
    ztab[z, 0:1] = total_a
    ztab[z, 1:2] = total_b
    over_z = []
    lot, there = wire.lot(ztab.at[pl.ds(0, nz - 1)]), wire.arrival()
    for k in range(1, nz):
        over_z.append(
            lot.message(ztab.at[z], ztab.at[z], None, dev(z_=mod(z + k, nz)), there)
        )
        over_z[-1].start()
    arrived(there, ztab.at[pl.ds(0, nz - 1)])
    carry = jnp.zeros((1, ch), F32)
    for j in range(nz):
        carry = jnp.where(j < z, ztab[j, 0:1] * carry + ztab[j, 1:2], carry)
    carry = before_a * carry + before_b
    mixed[...] = ((decay * carry + driven) * acc[1, RIM:]).astype(BF16)
    w_in.step(1)
    w_down.step(1)

    loads["outw"].wait()
    columns = (xo, xn, xp, x)

    def block(i):
        return pl.ds(pl.multiple_of(i * cw, 128), cw)

    over_d2d = []
    lot = wire.lot(oi)
    for n, i in enumerate(columns):
        for core in (1 - c, c):
            at = pl.multiple_of((i * 2 + core) * cw, 128)
            part = jnp.dot(mixed[...], outw[:, pl.ds(at, cw)], preferred_element_type=F32)
            op[core, :, block(i)] = part.astype(BF16)
            if core is not c:
                over_d2d.append(lot.message(op.at[1 - c, :, block(i)], oi.at[n], oi.at[n], sibling))
                over_d2d[-1].start()

    out_ring = Gathered(wire.lot(obox), lambda i, h: op.at[c, pl.ds(h * hm, hm), block(i)], x, along_x, obox)
    starts = (out_ring.start_far, out_ring.start_next, out_ring.start_prev, lambda: None)
    for n, i in enumerate(columns):
        over_d2d[n].arrived()
        op[c, :, block(i)] = (op[c, :, block(i)].astype(F32) + oi[n].astype(F32)).astype(BF16)
        starts[n]()
    out_ring.relay()
    if steps > 2:
        w_in.step(2)
    for h, value in enumerate(out_ring.result()):
        rows = pl.ds(h * hm, hm)
        res[rows] = (x_ref[rows].astype(F32) + value).astype(BF16)

    hg = rm // GROUPS
    hh = hg // 2
    other = 1 - c

    def token(j, h=None):
        if h is None:
            return pl.ds(pl.multiple_of(j * hg, 16), hg)
        return pl.ds(pl.multiple_of(j * hg + h * hh, 16), hh)

    def of_core(core, g, size, h=0):
        return pl.ds(pl.multiple_of(core * rm + g * hg + h * hh, 16), size)

    here_rows = pl.ds(pl.multiple_of(y * hg, 16), hg)

    class Rows:
        def __init__(self, g):
            self.g = g
            there = xt.at[1 - c, g, here_rows, block(x)]
            lot = wire.lot(xt.at[0, :, pl.ds(0, 30 * hg // (NX * GROUPS))])
            self.swap = wire.lot(there).message(res.at[of_core(other, g, hg)], xt.at[c, g, here_rows, block(x)], there, sibling)
            size = lambda n: xt.at[0, 0, pl.ds(0, n * hg), pl.ds(0, cw)]
            self.b_far, self.size = wire.arrival(), size

            def ring(core, rows, wholes, columns_of, me, device_of, far=None):
                return Around(
                    lot,
                    lambda m, h: xt.at[core, g, rows(m, h), columns_of(m)],
                    lambda m: xt.at[core, g, wholes(m), columns_of(m)],
                    size, me, device_of, far,
                )

            def over_x(core, j, far=None):
                return ring(core, lambda m, h: token(j, h), lambda m: token(j), block, x, along_x, far)

            def over_y(core, i):
                return ring(core, token, token, lambda m: block(i), y, along_y)

            self.a_x, self.b_y = over_x(c, y), over_y(other, x)
            self.a_y = [over_y(c, i) for i in (x, xp, xn, xo)]
            self.b_x = [over_x(other, j, self.b_far) for j in (y, yp, yn, yo)]

        def begin(self):
            self.swap.start()
            xt[c, self.g, here_rows, block(x)] = res[of_core(c, self.g, hg)]
            self.a_x.start()

        def begin_other(self):
            self.swap.arrived()
            self.b_y.start()

        def own(self):
            self.a_y[0].start()
            self.b_x[0].start()

        def relay_first(self):
            self.a_x.forward()
            self.b_y.forward()

        def sides(self):
            for n in (1, 2):
                self.a_y[n].start()
                self.b_x[n].start()

        def far(self):
            self.a_x.opp_done()
            self.a_y[3].start()
            self.b_y.opp_done()
            self.b_x[3].start()

        def relay(self, n):
            self.a_y[n].forward()
            self.b_x[n].forward()

        def a_done(self, n):
            self.a_y[n].opp_done()

        def b_done(self):
            arrived(self.b_far, self.size(4))

    class Sums:
        def __init__(self, g):
            self.g = g
            lot = wire.lot(po.at[0, :, pl.ds(0, 60 * hh // (NX * GROUPS))])
            self.a = [
                Gathered(lot, lambda j, h, i=i: po.at[c, g, token(j, h), block(i)], y, along_y, abox.at[g, n])
                for n, i in enumerate(columns)
            ]
            self.b = [
                Gathered(lot, lambda i, h, j=j: po.at[other, g, token(j, h), block(i)], x, along_x, bbox.at[g, n])
                for n, j in enumerate(b_rows)
            ]
            self.a_last = Gathered(lot, lambda i, h: po.at[c, g, token(y, h), block(i)], x, along_x, abox2.at[g])
            self.b_last = Gathered(lot, lambda j, h: po.at[other, g, token(j, h), block(x)], y, along_y, bbox2.at[g])
            self.back = wire.lot(give.at[g]).message(give.at[g], got.at[g], got.at[g], sibling)

        def a_all(self, n):
            self.a[n].start_far()
            self.a[n].start_next()
            self.a[n].start_prev()

        def b_all(self, method):
            for ring in self.b:
                getattr(ring, method)()

        def down(self):
            starts = (
                lambda: (self.a_all(0), self.b_all("start_far")),
                lambda: (self.a_all(1), self.b_all("start_next")),
                lambda: (self.a_all(2), self.b_all("start_prev")),
                lambda: self.a_all(3),
            )

            def one(k, _):
                i = picked(k, list(columns))
                both = pl.ds(pl.multiple_of(i * 2 * cw, 128), 2 * cw)
                part = jnp.dot(hid[...], wt[2, :, both], preferred_element_type=F32).astype(BF16)
                for core in range(2):
                    po[core, self.g, :, block(i)] = part[:, core * cw : (core + 1) * cw]
                at_step(k, dict(enumerate(starts)))
                return 0

            lax.fori_loop(0, 4, one, 0)

        def relay(self, n):
            self.a[n].relay()
            self.b[n].relay()

        def first_sums(self):
            a_starts = (self.a_last.start_far, self.a_last.start_next, self.a_last.start_prev, lambda: None)
            b_starts = (self.b_last.start_far, self.b_last.start_next, self.b_last.start_prev, lambda: None)
            for n in range(4):
                for ring, start, core, rows_at, i in (
                    (self.a[n], a_starts[n], c, y, columns[n]),
                    (self.b[n], b_starts[n], other, b_rows[n], x),
                ):
                    for h, value in enumerate(ring.result()):
                        po[core, self.g, token(rows_at, h), block(i)] = value.astype(BF16)
                    start()

        def relay_last(self):
            self.b_last.relay()
            self.a_last.relay()

        def results(self):
            for h, value in enumerate(self.b_last.result()):
                give[self.g, pl.ds(h * hh, hh)] = value.astype(BF16)
            self.back.start()
            for h, value in enumerate(self.a_last.result()):
                rows = of_core(c, self.g, hh, h)
                o_ref[rows] = (res[rows].astype(F32) + value).astype(BF16)

        def others(self):
            self.back.arrived()
            rows = of_core(other, self.g, hg)
            o_ref[rows] = (res[rows].astype(F32) + got[self.g].astype(F32)).astype(BF16)

    b_rows = (yo, yn, yp, y)
    rows_0, rows_1 = Rows(0), Rows(1)
    sums_0, sums_1 = Sums(0), Sums(1)

    def multiply(rows, extra):
        pairs = (((c, x), (other, x)), ((c, xp), (c, xn)), ((other, xp), (other, xn)), ((c, xo), (other, xo)))
        waits = {
            0: lambda: rows.a_done(0),
            1: lambda: (rows.a_done(1), rows.a_done(2)),
            3: lambda: (rows.a_done(3), rows.b_done()),
        }
        acc2[...] = jnp.zeros_like(acc2)
        ss2[...] = jnp.zeros_like(ss2)

        def one(k, _):
            at_step(k, extra)
            at_step(k, waits)
            scaled, weights, squares = [], [], 0.0
            for n in range(2):
                core, i = picked(k, [w[n][0] for w in pairs]), picked(k, [w[n][1] for w in pairs])
                at = pl.multiple_of((i * 2 + core) * cw, 128)
                block_rows = xt[core, rows.g, :, block(i)].astype(F32)
                squares = squares + lane_sums(block_rows * block_rows)
                scaled.append((block_rows * mg_ref[:, pl.ds(at, cw)]).astype(BF16))
                weights.append(wt[0:2, :, pl.ds(at, cw)].reshape(4 * ff, cw))
            ss2[...] += squares
            acc2[...] += lax.dot_general(
                jnp.concatenate(scaled, axis=1), jnp.concatenate(weights, axis=1), (((1,), (1,)), ((), ())),
                preferred_element_type=F32,
            )
            return 0

        lax.fori_loop(0, 4, one, 0)
        scale2 = lax.rsqrt(jnp.sum(ss2[...], axis=1, keepdims=True) * (1.0 / d) + EPS)
        hid[...] = (jax.nn.gelu(acc2[:, : 2 * ff] * scale2, approximate=True) * (acc2[:, 2 * ff :] * scale2)).astype(BF16)

    rows_0.begin()
    rows_0.begin_other()
    rows_0.own()
    rows_1.begin()
    rows_1.begin_other()
    rows_0.relay_first()
    rows_0.sides()
    rows_0.far()
    for k in range(3, steps):
        w_in.step(k)
    rows_0.relay(0)
    if steps > 2:
        w_down.step(2)
    rows_1.relay_first()
    rows_0.relay(1)
    rows_1.own()
    rows_0.relay(2)
    rows_1.sides()
    rows_0.relay(3)
    rows_1.far()
    w_in.step(steps)
    for k in range(3, steps):
        w_down.step(k)
    w_in.finish()
    multiply(rows_0, {n: functools.partial(rows_1.relay, n) for n in range(4)})
    w_down.step(steps)
    w_down.finish()
    sums_0.down()
    multiply(rows_1, {n + 1: functools.partial(sums_0.relay, n) for n in range(3)})
    sums_0.relay(3)
    sums_1.down()
    sums_0.first_sums()
    for n in range(4):
        sums_1.relay(n)
    sums_0.relay_last()
    sums_1.first_sums()
    sums_0.results()
    sums_1.relay_last()
    sums_0.others()
    sums_1.results()
    sums_1.others()
    wire.drain()


def shards(
    nz, layer_input, norm_gain, in_weights, conv_weight, conv_bias, gate_weights, gate_bias, decay_rate, out_weight,
    mlp_gain, mlp_in, mlp_out,
):
    tm, cw = layer_input.shape
    d, ch = in_weights.shape[1:]
    units = mlp_out.shape[0]
    ff = units // NY
    hg = tm // 2 // GROUPS
    vmem = pl.BlockSpec(memory_space=pltpu.VMEM)
    hbm = pl.BlockSpec(memory_space=pl.ANY)
    scratch = [
        ((8, RIM + tm, cw), BF16),
        ((2, d, ch), BF16),
        ((ch, d), BF16),
        (mlp_in.shape, BF16),
        ((3, units, mlp_in.shape[1]), BF16),
        ((3, 2 * ff, d), BF16),
        ((2, RIM + tm, ch), F32),
        ((RIM + tm, 128), F32),
        ((NY, 2, ch), F32),
        ((nz, 2, ch), F32),
        ((tm, ch), BF16),
        ((2, tm, NX * cw), BF16),
        ((4, tm, cw), BF16),
        ((6, tm // 2, cw), BF16),
        ((tm, cw), BF16),
        ((2, GROUPS, NY * hg, NX * cw), BF16),
        ((NY * hg, 4 * ff), F32),
        ((NY * hg, 128), F32),
        ((NY * hg, 2 * ff), BF16),
        ((2, GROUPS, NY * hg, NX * cw), BF16),
        ((GROUPS, 4, 6, hg // 2, cw), BF16),
        ((GROUPS, 4, 6, hg // 2, cw), BF16),
        ((GROUPS, 6, hg // 2, cw), BF16),
        ((GROUPS, 6, hg // 2, cw), BF16),
        ((GROUPS, hg, cw), BF16),
        ((GROUPS, hg, cw), BF16),
    ]
    call = pl.pallas_call(
        functools.partial(kernel, nz),
        out_shape=jax.ShapeDtypeStruct((tm, cw), BF16),
        in_specs=[vmem] * 8 + [hbm] * 4,
        out_specs=vmem,
        scratch_shapes=[pltpu.VMEM(shape, dtype) for shape, dtype in scratch]
        + [
            pltpu.SemaphoreType.DMA((LOTS,)),
            pltpu.SemaphoreType.DMA((ARRIVALS,)),
            pltpu.SemaphoreType.DMA((4,)),
        ],
        compiler_params=pltpu.CompilerParams(
            collective_id=0, has_side_effects=True, vmem_limit_bytes=56 * 1024 * 1024
        ),
    )
    return call(
        layer_input, norm_gain[None], conv_weight, conv_bias[None], gate_weights, gate_bias, decay_rate[None],
        mlp_gain[None], in_weights, out_weight, mlp_in, mlp_out,
    )


def solution(mesh):
    return jax.shard_map(
        functools.partial(shards, mesh.shape["seq"] // NY),
        mesh=mesh,
        in_specs=(
            P("seq", "tensor"),
            P(),
            P(None, None, "tensor"),
            P(None, "tensor"),
            P("tensor"),
            P(None, "tensor", None, None),
            P(None, "tensor"),
            P("tensor"),
            P("tensor", None),
            P(),
            P(None, "seq", "tensor"),
            P("tensor", "seq"),
        ),
        out_specs=P("seq", "tensor"),
        check_vma=False,
    )
```
